32 devices in a mesh: dp: 4 (over y, x), ctx: 2 (over core), tensor: 4 (over z).
Axes of the slice: x: 2, y: 2, z: 4, core: 2. Of those that a mesh axis runs over, the one named last changes fastest.
Arguments:
- block_in: bfloat16 [2048, 4, 1536], P(('ctx', 'tensor'), 'dp'), may hold values from -6 to 6
- cotangent: bfloat16 [2048, 4, 1536], P(('ctx', 'tensor'), 'dp'), may hold values from -6 to 6
- segments: int32 [4, 2048], P('dp', 'ctx'), may hold values from 0 to 7, never falling along the last dimension, each value on 1 to 1024 neighbouring positions
- norm_gain: float32 [1536], replicated, may hold values from 0.5 to 1.5
- inward_weight: float32 [1536, 2, 3072], P(('dp', 'ctx'), None, 'tensor'), may hold values from -0.15625 to 0.15625
- shared_weight: float32 [1536, 304], replicated, may hold values from -0.15625 to 0.15625
- conv_filter: float32 [5, 3328], replicated, may hold values from -3 to 3
- head_params: float32 [3, 48], replicated, may hold values from -12 to 1.5, as said below
- gated_gain: float32 [3072], replicated, may hold values from 0.5 to 1.5
- exit_weight: float32 [1536, 3072], P(('dp', 'ctx'), 'tensor'), may hold values from -0.109375 to 0.109375
- norm_first: float32 [1536], replicated, may hold values from -56 to 56
- norm_second: float32 [1536], replicated, may hold values from 262.144 to 4177.92
- entry_first: float32 [1536, 2, 3072], P(('dp', 'ctx'), None, 'tensor'), may hold values from -56 to 56
- entry_second: float32 [1536, 2, 3072], P(('dp', 'ctx'), None, 'tensor'), may hold values from 262.144 to 4177.92
- shared_first: float32 [1536, 304], replicated, may hold values from -64 to 64
- shared_second: float32 [1536, 304], replicated, may hold values from 311.296 to 4997.12
- filter_first: float32 [5, 3328], replicated, may hold values from -48 to 48
- filter_second: float32 [5, 3328], replicated, may hold values from 180.224 to 2949.12
- head_first: float32 [3, 48], replicated, may hold values from -128 to 128
- head_second: float32 [3, 48], replicated, may hold values from 1638.4 to 26214.4
- gated_first: float32 [3072], replicated, may hold values from -64 to 64
- gated_second: float32 [3072], replicated, may hold values from 425.984 to 6799.36
- exit_first: float32 [1536, 3072], P(('dp', 'ctx'), 'tensor'), may hold values from -112 to 112
- exit_second: float32 [1536, 3072], P(('dp', 'ctx'), 'tensor'), may hold values from 1064.96 to 17203.2
Outputs:
- block_output: bfloat16 [2048, 4, 1536], P(('ctx', 'tensor'), 'dp')
- input_grad: float32 [2048, 4, 1536], P(('ctx', 'tensor'), 'dp')
- norm_grad: float32 [1536], replicated
- norm_new: float32 [1536], replicated
- norm_first_new: float32 [1536], replicated
- norm_second_new: float32 [1536], replicated
- entry_grad: float32 [1536, 2, 3072], P(('dp', 'ctx'), None, 'tensor')
- entry_new: float32 [1536, 2, 3072], P(('dp', 'ctx'), None, 'tensor')
- entry_first_new: float32 [1536, 2, 3072], P(('dp', 'ctx'), None, 'tensor')
- entry_second_new: float32 [1536, 2, 3072], P(('dp', 'ctx'), None, 'tensor')
- shared_grad: float32 [1536, 304], replicated
- shared_new: float32 [1536, 304], replicated
- shared_first_new: float32 [1536, 304], replicated
- shared_second_new: float32 [1536, 304], replicated
- filter_grad: float32 [5, 3328], replicated
- filter_new: float32 [5, 3328], replicated
- filter_first_new: float32 [5, 3328], replicated
- filter_second_new: float32 [5, 3328], replicated
- head_grad: float32 [3, 48], replicated
- head_new: float32 [3, 48], replicated
- head_first_new: float32 [3, 48], replicated
- head_second_new: float32 [3, 48], replicated
- gated_grad: float32 [3072], replicated
- gated_new: float32 [3072], replicated
- gated_first_new: float32 [3072], replicated
- gated_second_new: float32 [3072], replicated
- exit_grad: float32 [1536, 3072], P(('dp', 'ctx'), 'tensor')
- exit_new: float32 [1536, 3072], P(('dp', 'ctx'), 'tensor')
- exit_first_new: float32 [1536, 3072], P(('dp', 'ctx'), 'tensor')
- exit_second_new: float32 [1536, 3072], P(('dp', 'ctx'), 'tensor')
The draws below stay inside these ranges and needn't reach their ends.
Inputs may be any that keep to these rules, and one draw needn't show every extreme that they name: `segments`: along a sequence the document numbers never fall; a document has 1 to 1024 tokens. `head_params`: row 0 holds each head's step size bias, from -1.5 to 0.5; row 1 the logarithm of its decay rate, from log(0.1 / 2048) to -2.7; row 2 its skip gain, from 0.5 to 1.5.
All inputs are finite; a program needn't handle non-finite values.
Results may differ from the reference program's by a relative error of at most 0.0035.
The reference program's roundings to bfloat16 on the way count: a program that leaves them out, or rounds other values in their place, can miss the bound.
Values may be sent and summed in bfloat16 or wider, within the bound.
A program may use at most 256 MiB of HBM per device.

```python
import math
import jax
import jax.numpy as jnp
import numpy as np
from jax import lax

D = 1536
HEADS = 48
HEAD_DIM = 64
STATE = 128
CONV = 4
SPAN = 256
STEP = 2
DI = 3072
SEQ_LEN = 2048
SEQS = 4
SEGS = 8
N_TENSOR = 4


def draw_head_params(key, part):
    streams = jax.random.split(key, 3)
    shift_row = jax.random.uniform(streams[0], (HEADS,), jnp.float32, -1.5, 0.5)
    rate_row = jax.random.uniform(streams[1], (HEADS,), jnp.float32, math.log(0.1 / SEQ_LEN), math.log(1.0 / 15.0))
    skip_row = jax.random.uniform(streams[2], (HEADS,), jnp.float32, 0.5, 1.5)
    return jnp.stack([shift_row, rate_row, skip_row])


def block_levels(stream_key, shape, cuts, low, top_value):
    loudness, own = 1.0, jax.random.fold_in(stream_key, 6)
    for position, shards_of in cuts:
        draws = jnp.exp(jax.random.uniform(jax.random.fold_in(own, position), (shards_of,), jnp.float32, low / len(cuts), top_value / len(cuts)))
        loudness = loudness * jnp.repeat(draws, shape[position] // shards_of).reshape([-1 if axis == position else 1 for axis in range(len(shape))])
    return loudness


def length_profile(amount, total, reach, lean):
    portions = [(1 << 20) // math.isqrt(grade ** lean) + 1 for grade in range(2, amount + 1)]
    rest, given = total - reach - (amount - 1), [1] * (amount - 1)
    while rest > 0:
        movable = [i for i in range(amount - 1) if given[i] < reach]
        mass, remaining = sum([portions[i] for i in movable]), rest
        for i in movable:
            extra = min(reach - given[i], max(1, remaining * portions[i] // mass), rest)
            given[i] = given[i] + extra
            rest = rest - extra
    return np.array([reach] + given)


def uneven_parts(key, amount, total, limit, slope):
    if amount == 2:
        one = jax.random.randint(key, (), max(1, total - limit), min(limit, total - 1) + 1)
        return jnp.stack([one, total - one])
    tallies = jnp.asarray(length_profile(amount, total, limit, slope), jnp.int32)
    twos = (amount - 1) // 2
    source_of, taker = tallies[1:1 + 2 * twos:2], tallies[2:2 + 2 * twos:2]
    slack = jnp.minimum(source_of - 1, limit - taker)
    passed = jax.random.randint(jax.random.fold_in(key, 1), (twos,), 0, 1 << 20) % (slack + 1)
    tallies = tallies.at[1:1 + 2 * twos:2].set(source_of - passed).at[2:2 + 2 * twos:2].set(taker + passed)
    return tallies[jax.random.permutation(jax.random.fold_in(key, 2), amount)]


def scatter_about(own_key, extent, deviation, most, cuts=(), held_as=jnp.bfloat16):
    values = jax.random.normal(own_key, extent, jnp.float32) * deviation
    if len(cuts) > 0:
        values = block_levels(own_key, extent, cuts, -0.22, 0.18) * values
    return jnp.clip(values, min=-most, max=most).astype(held_as)


def setup_inputs(seed: int = 0) -> dict:
    streams_of = jax.random.split(jax.random.key(seed), 25)
    block_in = scatter_about(streams_of[0], (SEQ_LEN, SEQS, D), 1.0, 6.0, ((0, 8), (1, 4)))
    cotangent = scatter_about(streams_of[1], (SEQ_LEN, SEQS, D), 1.0, 6.0, ((0, 8), (1, 4)))
    segments = jax.vmap(lambda own: jnp.searchsorted(jnp.cumsum(uneven_parts(own, SEGS, SEQ_LEN, SEQ_LEN // 2, 1)), jnp.arange(SEQ_LEN), side="right"))(jax.random.split(streams_of[2], SEQS)).reshape((SEQS, SEQ_LEN)).astype(jnp.int32)
    norm_gain = jnp.clip(1.0 + 0.1 * jax.random.normal(streams_of[3], (D,), jnp.float32), 0.5, 1.5)
    inward_weight = scatter_about(streams_of[4], (D, 2, DI), D ** -0.5, 0.15625, ((0, 8), (2, 4)), jnp.float32)
    shared_weight = scatter_about(streams_of[5], (D, 2 * STATE + HEADS), D ** -0.5, 0.15625, (), jnp.float32)
    conv_filter = scatter_about(streams_of[6], (CONV + 1, DI + 2 * STATE), 4 ** -0.5, 3.0, (), jnp.float32)
    head_params = draw_head_params(jax.random.fold_in(streams_of[24], 71), 0)
    gated_gain = jnp.clip(1.0 + 0.1 * jax.random.normal(streams_of[8], (DI,), jnp.float32), 0.5, 1.5)
    exit_weight = scatter_about(streams_of[9], (D, DI), DI ** -0.5, 0.109375, ((0, 8), (1, 4)), jnp.float32)
    norm_first = scatter_about(streams_of[10], (D,), (0.1 * (SEQ_LEN * SEQS) ** 0.5), 56.0, (), jnp.float32)
    norm_second = jnp.clip(jnp.exp(jax.random.uniform(streams_of[11], (D,), jnp.float32, math.log(262.144), math.log(4177.92))), 262.144, 4177.92)
    entry_first = scatter_about(streams_of[12], (D, 2, DI), (0.1 * (SEQ_LEN * SEQS) ** 0.5), 56.0, ((0, 8), (2, 4)), jnp.float32)
    entry_second = jnp.clip(jnp.exp(math.log(4177.92) - 2.7686748 * jax.random.uniform(streams_of[13], (D, 2, DI), jnp.float32) ** block_levels(streams_of[13], (D, 2, DI), ((0, 8), (2, 4)), -0.2, 0.2)), 262.144, 4177.92)
    shared_first = scatter_about(streams_of[14], (D, 2 * STATE + HEADS), (0.11 * (SEQ_LEN * SEQS) ** 0.5), 64.0, (), jnp.float32)
    shared_second = jnp.clip(jnp.exp(jax.random.uniform(streams_of[15], (D, 2 * STATE + HEADS), jnp.float32, math.log(311.296), math.log(4997.12))), 311.296, 4997.12)
    filter_first = scatter_about(streams_of[16], (CONV + 1, DI + 2 * STATE), (0.084 * (SEQ_LEN * SEQS) ** 0.5), 48.0, (), jnp.float32)
    filter_second = jnp.clip(jnp.exp(jax.random.uniform(streams_of[17], (CONV + 1, DI + 2 * STATE), jnp.float32, math.log(180.224), math.log(2949.12))), 180.224, 2949.12)
    head_first = scatter_about(streams_of[18], (3, HEADS), (0.25 * (SEQ_LEN * SEQS) ** 0.5), 128.0, (), jnp.float32)
    head_second = jnp.clip(jnp.exp(jax.random.uniform(streams_of[19], (3, HEADS), jnp.float32, math.log(1638.4), math.log(26214.4))), 1638.4, 26214.4)
    gated_first = scatter_about(streams_of[20], (DI,), (0.13 * (SEQ_LEN * SEQS) ** 0.5), 64.0, (), jnp.float32)
    gated_second = jnp.clip(jnp.exp(jax.random.uniform(streams_of[21], (DI,), jnp.float32, math.log(425.984), math.log(6799.36))), 425.984, 6799.36)
    exit_first = scatter_about(streams_of[22], (D, DI), (0.2 * (SEQ_LEN * SEQS) ** 0.5), 112.0, ((0, 8), (1, 4)), jnp.float32)
    exit_second = jnp.clip(jnp.exp(math.log(17203.2) - 2.7821582 * jax.random.uniform(streams_of[23], (D, DI), jnp.float32) ** block_levels(streams_of[23], (D, DI), ((0, 8), (1, 4)), -0.2, 0.2)), 1064.96, 17203.2)
    return {"block_in": block_in, "cotangent": cotangent, "segments": segments, "norm_gain": norm_gain, "inward_weight": inward_weight, "shared_weight": shared_weight, "conv_filter": conv_filter, "head_params": head_params, "gated_gain": gated_gain, "exit_weight": exit_weight, "norm_first": norm_first, "norm_second": norm_second, "entry_first": entry_first, "entry_second": entry_second, "shared_first": shared_first, "shared_second": shared_second, "filter_first": filter_first, "filter_second": filter_second, "head_first": head_first, "head_second": head_second, "gated_first": gated_first, "gated_second": gated_second, "exit_first": exit_first, "exit_second": exit_second}


@jax.custom_vjp
def low(v):
    return lax.optimization_barrier(v.astype(jnp.bfloat16)).astype(jnp.float32)

@jax.custom_vjp
def low_back(v):
    return v

def low_keep(v):
    return (low(v), None)

def low_pass(kept, grad):
    return (grad,)

def back_keep(v):
    return (v, None)

def back_low(kept, grad):
    return (low(grad),)
low.defvjp(low_keep, low_pass)
low_back.defvjp(back_keep, back_low)
norm_eps = 1e-05
beta_first = 0.9
beta_second = 0.95
adam_eps = 1e-08
rate_matrix = 0.01
rate_vector = 0.4
decay_matrix = 0.1
topmost_precision = lax.Precision.HIGHEST

def pad_rows(values):
    return jnp.concatenate([jnp.zeros((CONV - 1,) + values.shape[1:], values.dtype), values], axis=0)

def conv_apply(padded, seg_pad, taps, bias):
    length = padded.shape[0] - (CONV - 1)
    seg_ids = seg_pad[CONV - 1:]
    total = bias
    for offset in range(CONV):
        same = (seg_pad[offset:offset + length] == seg_ids).astype(jnp.float32)[..., None]
        total = total + taps[offset] * padded[offset:offset + length] * same
    return jax.nn.silu(total)

def span_step(state, pieces):
    values, b_proj, c_proj, delta, logdec, seg_ids, prev_id = pieces
    cumulative = jnp.cumsum(logdec, axis=0)
    length = seg_ids.shape[0]
    order = jnp.arange(length)
    allowed = ((seg_ids[:, None] == seg_ids[None, :]) & (order[:, None] >= order[None, :])).astype(jnp.float32)
    spread = cumulative[:, None, :] - cumulative[None, :, :]
    kernel = jnp.exp(jnp.where(allowed[..., None] > 0, spread, 0.0)) * allowed[..., None]
    scores = jnp.dot(c_proj, b_proj.T, precision=topmost_precision)
    mixing = scores[..., None] * kernel * delta[None]
    outputs = jnp.einsum('tsh,shp->thp', mixing, values, precision=topmost_precision)
    inflow = (seg_ids == prev_id).astype(jnp.float32)[:, None]
    outputs = outputs + jnp.einsum('tn,hpn->thp', c_proj, state, precision=topmost_precision) * (jnp.exp(cumulative) * inflow)[..., None]
    keeping = (seg_ids == seg_ids[-1]).astype(jnp.float32)[:, None]
    tail = jnp.exp(cumulative[-1][None] - cumulative) * keeping * delta
    carry_on = jnp.exp(cumulative[-1]) * (seg_ids[-1] == prev_id).astype(jnp.float32)
    new_state = carry_on[:, None, None] * state + jnp.einsum('sh,shp,sn->hpn', tail, values, b_proj, precision=topmost_precision)
    return (new_state, outputs)

def ssd_sequence(values, b_proj, c_proj, delta, logdec, seg_ids):
    count = seg_ids.shape[0] // SPAN

    def split(array):
        return array.reshape((count, SPAN) + array.shape[1:])
    seg_blocks = split(seg_ids)
    prev_ids = jnp.concatenate([jnp.full((1,), -1, jnp.int32), seg_blocks[:-1, -1].astype(jnp.int32)])
    start = jnp.zeros((values.shape[1], HEAD_DIM, STATE), jnp.float32)
    final, outputs = lax.scan(jax.checkpoint(span_step), start, (split(values), split(b_proj), split(c_proj), split(delta), split(logdec), seg_blocks, prev_ids))
    return outputs.reshape(values.shape)

def forward(inputs, norm_gain, inward_weight, shared_weight, conv_filter, head_params, gated_gain, exit_weight, segments):
    scale_in = lax.rsqrt(lax.optimization_barrier(jnp.mean(inputs * inputs, axis=-1, keepdims=True)) + norm_eps)
    normalized_input = low(inputs * scale_in * norm_gain)
    inward_projection = jnp.einsum('fzo,ogv->fzgv', normalized_input, low(inward_weight), precision=topmost_precision)
    gate_in = low_back(inward_projection[:, :, 0])
    inner = low(low_back(inward_projection[:, :, 1]))
    shared = jnp.einsum('lsd,dk->lsk', normalized_input, low(shared_weight), precision=topmost_precision)
    delta_raw = low_back(shared[..., 2 * STATE:])
    seg_rows = segments.T.astype(jnp.int32)
    seg_pad = jnp.concatenate([jnp.full((CONV - 1, seg_rows.shape[1]), -1, jnp.int32), seg_rows], axis=0)
    inner_act = conv_apply(pad_rows(inner), seg_pad, conv_filter[:CONV, :DI], conv_filter[CONV, :DI])
    delta = jax.nn.softplus(delta_raw + head_params[0])
    logdec = -jnp.exp(head_params[1]) * delta
    per_group = HEADS // N_TENSOR
    group_outputs = []
    for group in range(N_TENSOR):
        bc_copy = low(low_back(shared[..., :2 * STATE]))
        bc_act = conv_apply(pad_rows(bc_copy), seg_pad, conv_filter[:CONV, DI:], conv_filter[CONV, DI:])
        first = group * per_group
        values = inner_act[..., first * HEAD_DIM:(first + per_group) * HEAD_DIM].reshape(SEQ_LEN, SEQS, per_group, HEAD_DIM)
        items = (values, bc_act[..., :STATE], bc_act[..., STATE:], delta[..., first:first + per_group], logdec[..., first:first + per_group], seg_rows)
        moved = tuple((jnp.moveaxis(item, 1, 0) for item in items))
        scanned = lax.map(lambda item: ssd_sequence(*item), moved)
        group_outputs.append(jnp.moveaxis(scanned, 0, 1) + head_params[2, first:first + per_group][:, None] * values)
    mixed_heads = jnp.concatenate(group_outputs, axis=2).reshape(SEQ_LEN, SEQS, DI)
    gated = mixed_heads * jax.nn.silu(gate_in)
    gate_scale = lax.rsqrt(lax.optimization_barrier(jnp.mean(gated * gated, axis=-1, keepdims=True)) + norm_eps)
    gnorm = low(gated * gate_scale * gated_gain)
    mixed = jnp.einsum('lsi,di->lsd', gnorm, low(exit_weight), precision=topmost_precision)
    return inputs + mixed

def adamw(weight, grad, first, second, rate, decay):
    first_new = beta_first * first + (1.0 - beta_first) * grad
    second_new = beta_second * second + (1.0 - beta_second) * grad * grad
    first_hat = first_new / (1.0 - beta_first ** STEP)
    second_hat = second_new / (1.0 - beta_second ** STEP)
    weight_new = weight - rate * (first_hat / (jnp.sqrt(second_hat) + adam_eps) + decay * weight)
    return (grad, weight_new, first_new, second_new)

def reference(block_in, cotangent, segments, norm_gain, inward_weight, shared_weight, conv_filter, head_params, gated_gain, exit_weight, norm_first, norm_second, entry_first, entry_second, shared_first, shared_second, filter_first, filter_second, head_first, head_second, gated_first, gated_second, exit_first, exit_second):
    inputs = block_in.astype(jnp.float32)
    norm_gain = norm_gain.astype(jnp.float32)
    inward_weight = inward_weight.astype(jnp.float32)
    shared_weight = shared_weight.astype(jnp.float32)
    conv_filter = conv_filter.astype(jnp.float32)
    head_params = head_params.astype(jnp.float32)
    gated_gain = gated_gain.astype(jnp.float32)
    exit_weight = exit_weight.astype(jnp.float32)
    seg_ids_all = segments.astype(jnp.int32)

    def wrapped(inputs, norm_gain, inward_weight, shared_weight, conv_filter, head_params, gated_gain, exit_weight):
        return forward(inputs, norm_gain, inward_weight, shared_weight, conv_filter, head_params, gated_gain, exit_weight, seg_ids_all)
    result, pullback = jax.vjp(wrapped, inputs, norm_gain, inward_weight, shared_weight, conv_filter, head_params, gated_gain, exit_weight)
    grads = pullback(cotangent.astype(jnp.float32))
    norm_set = adamw(norm_gain, grads[1], norm_first.astype(jnp.float32), norm_second.astype(jnp.float32), rate_vector, 0.0)
    entry_set = adamw(inward_weight, grads[2], entry_first.astype(jnp.float32), entry_second.astype(jnp.float32), rate_matrix, decay_matrix)
    shared_set = adamw(shared_weight, grads[3], shared_first.astype(jnp.float32), shared_second.astype(jnp.float32), rate_matrix, decay_matrix)
    filter_set = adamw(conv_filter, grads[4], filter_first.astype(jnp.float32), filter_second.astype(jnp.float32), rate_vector, 0.0)
    head_set = adamw(head_params, grads[5], head_first.astype(jnp.float32), head_second.astype(jnp.float32), rate_vector, 0.0)
    gated_set = adamw(gated_gain, grads[6], gated_first.astype(jnp.float32), gated_second.astype(jnp.float32), rate_vector, 0.0)
    exit_set = adamw(exit_weight, grads[7], exit_first.astype(jnp.float32), exit_second.astype(jnp.float32), rate_matrix, decay_matrix)
    return (result.astype(jnp.bfloat16), grads[0], norm_set[0], norm_set[1], norm_set[2], norm_set[3], entry_set[0], entry_set[1], entry_set[2], entry_set[3], shared_set[0], shared_set[1], shared_set[2], shared_set[3], filter_set[0], filter_set[1], filter_set[2], filter_set[3], head_set[0], head_set[1], head_set[2], head_set[3], gated_set[0], gated_set[1], gated_set[2], gated_set[3], exit_set[0], exit_set[1], exit_set[2], exit_set[3])
```

```python
import functools

import jax
import jax.numpy as jnp
from jax import lax
from jax.experimental import pallas as pl
from jax.experimental.pallas import tpu as pltpu
from jax.sharding import PartitionSpec as P

HEADS = 48
HEAD_DIM = 64
STATE = 128
CONV = 4
STEP = 2
DI = 3072
CHUNK = 128
LANES = 128

norm_eps = 1e-05
beta_first = 0.9
beta_second = 0.95
adam_eps = 1e-08
rate_matrix = 0.01
rate_vector = 0.4
decay_matrix = 0.1

MESH = pl.DeviceIdType.MESH
f32 = jnp.float32
bf16 = jnp.bfloat16
NT = (((1,), (1,)), ((), ()))
NEG = -1e30


def pick(index, table):
    out = jnp.int32(table[0])
    for i, v in enumerate(table[1:], 1):
        out = jnp.where(index == i, jnp.int32(v), out)
    return out


def gather_kernel(n_dp, n_ctx, n_z, ring, zc, n_ref, w_ref, nf, wf, halo, *sems):
    z_send, z_recv, d_send, d_recv, c_send, c_recv, h_sem, l_sem = sems
    z, d, c = lax.axis_index("tensor"), lax.axis_index("dp"), lax.axis_index("ctx")
    pos = pick(d, [ring.index(i) for i in range(n_dp)])
    nxt = pick(lax.rem(pos + 1, n_dp), ring)
    prv = pick(lax.rem(pos + n_dp - 1, n_dp), ring)
    c_next, c_prev = lax.rem(c + 1, n_ctx), lax.rem(c + n_ctx - 1, n_ctx)
    rows, wr = n_ref.shape[0], w_ref.shape[0]
    half, zr = wr // 2, rows // zc
    bar = pltpu.get_barrier_semaphore()

    @pl.when(z > 0)
    def _():
        pl.semaphore_signal(bar, device_id={"tensor": z - 1}, device_id_type=MESH)

    @pl.when(z < n_z - 1)
    def _():
        pl.semaphore_signal(bar, device_id={"tensor": z + 1}, device_id_type=MESH)

    pl.semaphore_signal(bar, device_id={"dp": nxt}, device_id_type=MESH)
    pl.semaphore_signal(bar, device_id={"dp": prv}, device_id_type=MESH)
    pl.semaphore_signal(bar, device_id={"ctx": c_prev}, device_id_type=MESH)
    if n_ctx > 2:
        pl.semaphore_signal(bar, device_id={"ctx": c_next}, device_id_type=MESH)
    extra = 3 if n_ctx == 2 else 4

    @pl.when((z > 0) & (z < n_z - 1))
    def _():
        pl.semaphore_wait(bar, extra + 2)

    @pl.when((z == 0) | (z == n_z - 1))
    def _():
        pl.semaphore_wait(bar, extra + 1)

    def zcopy(src, k, to, first, way):
        here = nf.at[pl.ds(src * rows + k * zr, zr)]
        return pltpu.make_async_remote_copy(
            n_ref.at[pl.ds(k * zr, zr)] if first else here,
            here,
            z_send.at[way, src, k],
            z_recv.at[src, k],
            device_id={"tensor": to},
            device_id_type=MESH,
        )

    def wpart(cc, dd, h):
        return wf.at[pl.ds((dd * n_ctx + cc) * wr + h * half, half)]

    def dcopy(sp, h, first):
        here = wpart(c, pick(sp, ring), h)
        return pltpu.make_async_remote_copy(
            w_ref.at[pl.ds(h * half, half)] if first else here,
            here,
            d_send.at[sp, h],
            d_recv.at[sp, h],
            device_id={"dp": nxt if h == 0 else prv},
            device_id_type=MESH,
        )

    def ccopy(cc, dd, h, first):
        here = wpart(cc, dd, h)
        return pltpu.make_async_remote_copy(
            w_ref.at[pl.ds(h * half, half)] if first else here,
            here,
            c_send.at[cc, dd, h],
            c_recv.at[cc, dd, h],
            device_id={"ctx": c_next},
            device_id_type=MESH,
        )

    def ring_pos(dist, h):
        return lax.rem(pos + (n_dp - dist if h == 0 else dist), n_dp)

    for k in range(zc):

        @pl.when(z < n_z - 1)
        def _(k=k):
            zcopy(z, k, z + 1, True, 0).start()

        @pl.when(z > 0)
        def _(k=k):
            zcopy(z, k, z - 1, True, 1).start()

        if k == 0:
            for h in range(2):
                dcopy(pos, h, True).start()
            for h in range(2):
                ccopy(c, d, h, True).start()
            own_w = pltpu.make_async_copy(
                w_ref, wf.at[pl.ds((d * n_ctx + c) * wr, wr)], l_sem.at[0]
            )
            own_n = pltpu.make_async_copy(n_ref, nf.at[pl.ds(z * rows, rows)], l_sem.at[1])
            own_w.start()
            own_n.start()
    for dist in range(1, max(n_z, n_dp)):
        for k in range(zc):
            if dist < n_z:

                @pl.when(z >= dist)
                def _(k=k, dist=dist):
                    zcopy(z - dist, k, z, False, 0).wait_recv()

                    @pl.when(z < n_z - 1)
                    def _():
                        zcopy(z - dist, k, z + 1, False, 0).start()

                @pl.when(z + dist < n_z)
                def _(k=k, dist=dist):
                    zcopy(z + dist, k, z, False, 1).wait_recv()

                    @pl.when(z > 0)
                    def _():
                        zcopy(z + dist, k, z - 1, False, 1).start()

            if k == 0 and dist < n_dp:
                for h in range(2):
                    sp = ring_pos(dist, h)
                    dcopy(sp, h, False).wait_recv()
                    if dist < n_dp - 1:
                        dcopy(sp, h, False).start()
                    ccopy(c, pick(sp, ring), h, False).start()
    own_n.wait()
    own_w.wait()
    edge = pltpu.make_async_remote_copy(
        nf.at[pl.ds(n_z * rows - halo.shape[0], halo.shape[0])],
        halo,
        h_sem.at[0],
        h_sem.at[1],
        device_id={"ctx": c_next},
        device_id_type=MESH,
    )
    edge.start()
    for step in range(1, n_ctx):
        cc = lax.rem(c + n_ctx - step, n_ctx)
        for dist in range(n_dp):
            for h in range(2):
                dd = pick(ring_pos(dist, h), ring)
                ccopy(cc, dd, h, False).wait_recv()
                if step < n_ctx - 1:
                    ccopy(cc, dd, h, False).start()
    edge.wait()
    for k in range(zc):
        for dist in range(n_z):

            @pl.when((z >= dist) & (z < n_z - 1))
            def _(k=k, dist=dist):
                zcopy(z - dist, k, z + 1, dist == 0, 0).wait_send()

            @pl.when((z + dist < n_z) & (z > 0))
            def _(k=k, dist=dist):
                zcopy(z + dist, k, z - 1, dist == 0, 1).wait_send()

    for dist in range(n_dp):
        for h in range(2):
            sp = ring_pos(dist, h)
            if dist < n_dp - 1:
                dcopy(sp, h, dist == 0).wait_send()
            for step in range(n_ctx - 1):
                cc = lax.rem(c + n_ctx - step, n_ctx)
                ccopy(cc, pick(sp, ring), h, dist == 0 and step == 0).wait_send()


def gather_all(dims, normed, weights):
    n_dp, n_ctx, n_z, ring = dims
    rows, width = normed.shape
    wr, wc = weights.shape
    zc = 2
    dma = pltpu.SemaphoreType.DMA
    return pl.pallas_call(
        functools.partial(gather_kernel, n_dp, n_ctx, n_z, ring, zc),
        out_shape=(
            jax.ShapeDtypeStruct((rows * n_z, width), normed.dtype),
            jax.ShapeDtypeStruct((wr * n_dp * n_ctx, wc), weights.dtype),
            jax.ShapeDtypeStruct((16, width), normed.dtype),
        ),
        in_specs=[pl.BlockSpec(memory_space=pltpu.VMEM)] * 2,
        out_specs=tuple([pl.BlockSpec(memory_space=pl.ANY)] * 3),
        scratch_shapes=[
            dma((2, n_z, zc)),
            dma((n_z, zc)),
            dma((n_dp, 2)),
            dma((n_dp, 2)),
            dma((n_ctx, n_dp, 2)),
            dma((n_ctx, n_dp, 2)),
            dma((2,)),
            dma((2,)),
        ],
        compiler_params=pltpu.CompilerParams(collective_id=0, has_side_effects=True),
        name="gather_all",
    )(normed, weights)


def all_sum_kernel(n_z, x_ref, o_ref, land, send, recv):
    z = lax.axis_index("tensor")
    bar = pltpu.get_barrier_semaphore()
    for k in range(1, n_z):
        pl.semaphore_signal(
            bar, device_id={"tensor": lax.rem(z + k, n_z)}, device_id_type=MESH
        )
    pl.semaphore_wait(bar, n_z - 1)
    copies = []
    for k in range(1, n_z):
        copy = pltpu.make_async_remote_copy(
            x_ref,
            land.at[k - 1],
            send.at[k - 1],
            recv.at[k - 1],
            device_id={"tensor": lax.rem(z + k, n_z)},
            device_id_type=MESH,
        )
        copy.start()
        copies.append(copy)
    for copy in copies:
        copy.wait()
    total = x_ref[...]
    for k in range(1, n_z):
        total = total + land[k - 1]
    o_ref[...] = total


def all_sum(n_z, collective_id, x):
    return pl.pallas_call(
        functools.partial(all_sum_kernel, n_z),
        out_shape=jax.ShapeDtypeStruct(x.shape, x.dtype),
        in_specs=[pl.BlockSpec(memory_space=pltpu.VMEM)],
        out_specs=pl.BlockSpec(memory_space=pltpu.VMEM),
        scratch_shapes=[
            pltpu.VMEM((n_z - 1,) + x.shape, x.dtype),
            pltpu.SemaphoreType.DMA((n_z - 1,)),
            pltpu.SemaphoreType.DMA((n_z - 1,)),
        ],
        compiler_params=pltpu.CompilerParams(collective_id=collective_id, has_side_effects=True),
        name="all_sum",
    )(x)


def split2(a):
    hi = a.astype(bf16)
    return hi, (a - hi.astype(f32)).astype(bf16)


def split3(a):
    hi = a.astype(bf16)
    rest = a - hi.astype(f32)
    mid = rest.astype(bf16)
    return hi, mid, (rest - mid.astype(f32)).astype(bf16)


def dot(a, b):
    return jnp.dot(a, b, preferred_element_type=f32)


def dot_nt(a, b):
    return lax.dot_general(a, b, NT, preferred_element_type=f32)


def lhs3(hi, lo):
    return jnp.concatenate([hi, lo, hi], axis=1)


def rhs3(hi, lo):
    return jnp.concatenate([hi, hi, lo], axis=0)


def rhs3_nt(hi, lo):
    return jnp.concatenate([hi, hi, lo], axis=1)


def left_half(shape):
    return lax.broadcasted_iota(jnp.int32, shape, 1) < HEAD_DIM


def expand(v, j):
    shape = (v.shape[0], LANES)
    return jnp.where(
        left_half(shape),
        jnp.broadcast_to(v[:, 2 * j : 2 * j + 1], shape),
        jnp.broadcast_to(v[:, 2 * j + 1 : 2 * j + 2], shape),
    )


def halves(a):
    keep = left_half(a.shape)
    return jnp.where(keep, a, 0.0), jnp.where(keep, 0.0, a)


def column(row):
    return jnp.broadcast_to(row, (LANES, LANES)).T


def ordered(length=CHUNK):
    r = lax.broadcasted_iota(jnp.int32, (length, length), 0)
    c = lax.broadcasted_iota(jnp.int32, (length, length), 1)
    return r, c


def fold8(a):
    out = a[0:8]
    for k in range(8, a.shape[0], 8):
        out = out + a[k : k + 8]
    return out


def head_columns(j):
    r, c = ordered(LANES)
    return jnp.where(c == 2 * j + jnp.where(r < HEAD_DIM, 0, 1), 1.0, 0.0).astype(bf16)


def sigmoid(x):
    return 1.0 / (1.0 + jnp.exp(-x))


def entry_kernel(
    nc,
    n_ref,
    w_ref,
    ws_ref,
    halo_ref,
    tok_ref,
    flag_ref,
    par_ref,
    cf_ref,
    gate_ref,
    v_ref,
    u_ref,
    act_ref,
    del_ref,
    cum_ref,
    sig_ref,
    s0_ref,
    fin_ref,
    thr_ref,
    vh_ref,
    vbuf,
    state,
    total,
):
    i = pl.program_id(0)
    rows = n_ref.shape[0]
    width = gate_ref.shape[1]
    cols = v_ref.shape[1]

    @pl.when(i == 0)
    def _():
        hv = jnp.concatenate(
            [dot(halo_ref[...], w_ref[:, width:]), dot(halo_ref[...], ws_ref[:, : 2 * STATE])],
            axis=1,
        )
        hv = hv.astype(bf16).astype(f32) * par_ref[3:4, 0:1]
        vbuf[0:8] = hv[8:16]
        vh_ref[...] = hv[8:16]
        state[...] = jnp.zeros_like(state)
        total[...] = jnp.zeros_like(total)

    @pl.when(i > 0)
    def _():
        vbuf[0:8] = vbuf[rows : rows + 8]

    n = n_ref[...]
    gate_ref[...] = dot(n, w_ref[:, :width])
    vi = dot(n, w_ref[:, width:]).astype(bf16)
    v_ref[:, :width] = vi
    vbuf[8 : rows + 8, :width] = vi.astype(f32)
    sh = dot(n, ws_ref[...])
    vb = sh[:, : 2 * STATE].astype(bf16)
    v_ref[:, width:] = vb
    vbuf[8 : rows + 8, width:] = vb.astype(f32)
    raw = sh[:, 2 * STATE :] + par_ref[0:1, :]
    delta = jnp.maximum(raw, 0.0) + jnp.log1p(jnp.exp(-jnp.abs(raw)))
    del_ref[...] = delta
    sig_ref[...] = sigmoid(raw)
    logdec = par_ref[1:2, :] * delta

    masks = [jnp.broadcast_to(tok_ref[:, k : k + 1], (rows, LANES)) for k in range(3)]
    for j in range(cols // LANES):
        cs = slice(j * LANES, (j + 1) * LANES)
        u = cf_ref[4:5, cs] + cf_ref[3:4, cs] * vbuf[8 : 8 + rows, cs]
        for k in range(3):
            u = u + cf_ref[k : k + 1, cs] * vbuf[5 + k : 5 + k + rows, cs] * masks[k]
        u_ref[:, cs] = u
        act_ref[:, cs] = u * sigmoid(u)

    r, c = ordered()
    tri = jnp.where(r >= c, 1.0, 0.0).astype(bf16)
    tri3 = jnp.concatenate([tri, tri, tri], axis=1)
    for k in range(rows // CHUNK):
        ts = slice(k * CHUNK, (k + 1) * CHUNK)
        chunk = i * (rows // CHUNK) + k
        cum = dot(tri3, jnp.concatenate(split3(logdec[ts]), axis=0))
        cum_ref[ts] = cum
        last = cum[CHUNK - 1 : CHUNK]
        weight = jnp.exp(last - cum) * tok_ref[ts, 3:4] * delta[ts]
        carry = jnp.exp(last) * flag_ref[pl.ds(chunk, 1), :]
        thr_ref[pl.ds(chunk, 1), :] = jnp.exp(total[0:1]) * flag_ref[pl.ds(nc + chunk, 1), :]
        total[0:1] = total[0:1] + last
        bt = lhs3(*split2(act_ref[ts, width : width + STATE].T))
        for j in range(width // LANES):
            cs = slice(j * LANES, (j + 1) * LANES)
            s0_ref[k, :, cs] = state[:, cs]
            xw = act_ref[ts, cs] * expand(weight, j)
            state[:, cs] = state[:, cs] * expand(carry, j) + dot(bt, rhs3(*split2(xw)))

    @pl.when(i == pl.num_programs(0) - 1)
    def _():
        thr_ref[nc : nc + 8, :] = jnp.broadcast_to(
            jnp.exp(total[0:1]) * flag_ref[3 * nc : 3 * nc + 1, :], (8, LANES)
        )
        fin_ref[...] = state[...]


def run_entry(normed, weights, shared_ext, halo, tok, flags, par, cf, width):
    tokens, d = normed.shape
    rows = 256
    nc = tokens // CHUNK
    cols = width + 2 * STATE
    one = pl.Buffered(1)

    def whole(shape):
        return pl.BlockSpec(shape, lambda i: (0,) * len(shape), pipeline_mode=one)

    def by_row(w):
        return pl.BlockSpec((rows, w), lambda i: (i, 0))

    def out(shape, dt=f32):
        return jax.ShapeDtypeStruct(shape, dt)

    return pl.pallas_call(
        functools.partial(entry_kernel, nc),
        grid=(tokens // rows,),
        in_specs=[
            by_row(d),
            whole((d, 2 * width)),
            whole(shared_ext.shape),
            whole(halo.shape),
            by_row(tok.shape[1]),
            whole(flags.shape),
            whole(par.shape),
            whole(cf.shape),
        ],
        out_specs=(
            by_row(width),
            by_row(cols),
            by_row(cols),
            by_row(cols),
            by_row(LANES),
            by_row(LANES),
            by_row(LANES),
            pl.BlockSpec((rows // CHUNK, STATE, width), lambda i: (i, 0, 0)),
            whole((STATE, width)),
            whole((nc + 8, LANES)),
            whole((8, cols)),
        ),
        out_shape=(
            out((tokens, width)),
            out((tokens, cols), bf16),
            out((tokens, cols)),
            out((tokens, cols)),
            out((tokens, LANES)),
            out((tokens, LANES)),
            out((tokens, LANES)),
            out((nc, STATE, width)),
            out((STATE, width)),
            out((nc + 8, LANES)),
            out((8, cols)),
        ),
        scratch_shapes=[
            pltpu.VMEM((rows + 8, cols), f32),
            pltpu.VMEM((STATE, width), f32),
            pltpu.VMEM((8, LANES), f32),
        ],
        compiler_params=pltpu.CompilerParams(dimension_semantics=("arbitrary",)),
        name="entry",
    )(normed, weights, shared_ext, halo, tok, flags, par, cf)


def mix_kernel(
    act_ref,
    del_ref,
    cum_ref,
    tok_ref,
    segr_ref,
    s0_ref,
    sin_ref,
    thr_ref,
    gate_ref,
    gain_ref,
    mixed_ref,
    sq_ref,
):
    chunk = pl.program_id(0)
    width = gate_ref.shape[1]
    b = act_ref[:, width : width + STATE]
    c = act_ref[:, width + STATE :]
    bh, bl = split2(b)
    ch, cl = split2(c)
    c3 = lhs3(ch, cl)
    scores = dot_nt(c3, rhs3_nt(bh, bl))
    cum = cum_ref[...]
    cum_t = cum.T
    r, s = ordered()
    same = tok_ref[:, 5:6] == segr_ref[pl.ds(chunk, 1), :]
    bias = jnp.where(same & (r >= s), 0.0, NEG)
    delta = del_ref[...]
    ramp = jnp.exp(cum) * tok_ref[:, 4:5]
    thr = thr_ref[pl.ds(chunk, 1), :]
    squares = jnp.zeros((CHUNK, LANES), f32)
    for j in range(width // LANES):
        cs = slice(j * LANES, (j + 1) * LANES)
        x = act_ref[:, cs]
        his, los = [], []
        for h in (2 * j, 2 * j + 1):
            decay = jnp.exp(cum[:, h : h + 1] - cum_t[h : h + 1, :] + bias)
            hi, lo = split2(scores * decay)
            his.append(hi)
            los.append(lo)
        xh, xl = split2(x * expand(delta, j))
        zero = jnp.zeros_like(xh)
        keep = left_half(xh.shape)
        xh0, xh1 = jnp.where(keep, xh, zero), jnp.where(keep, zero, xh)
        xl0, xl1 = jnp.where(keep, xl, zero), jnp.where(keep, zero, xl)
        y = dot(
            jnp.concatenate(his + los + his, axis=1),
            jnp.concatenate([xh0, xh1, xh0, xh1, xl0, xl1], axis=0),
        )
        st = s0_ref[0, :, cs] + expand(thr, j) * sin_ref[:, cs]
        y = y + dot(c3, rhs3(*split2(st))) * expand(ramp, j)
        mixed = y + gain_ref[0:1, cs] * x
        mixed_ref[:, cs] = mixed
        g = gate_ref[:, cs]
        gated = mixed * (g * sigmoid(g))
        squares = squares + gated * gated
    ones = jnp.ones((8, 2 * LANES), bf16)
    sq_ref[pl.ds(chunk, 1), :] = dot_nt(ones, jnp.concatenate(split2(squares), axis=1))[0:1]


def run_mix(act, delta, cum, tok, segr, s0, s_in, thr, gate, gains):
    tokens, cols = act.shape
    width = gate.shape[1]
    nc = tokens // CHUNK

    def whole(shape):
        return pl.BlockSpec(shape, lambda i: (0,) * len(shape))

    def by_row(w):
        return pl.BlockSpec((CHUNK, w), lambda i: (i, 0))

    return pl.pallas_call(
        mix_kernel,
        grid=(nc,),
        in_specs=[
            by_row(cols),
            by_row(LANES),
            by_row(LANES),
            by_row(tok.shape[1]),
            whole(segr.shape),
            pl.BlockSpec((1, STATE, width), lambda i: (i, 0, 0)),
            whole(s_in.shape),
            whole(thr.shape),
            by_row(width),
            whole(gains.shape),
        ],
        out_specs=(by_row(width), whole((nc, LANES))),
        out_shape=(
            jax.ShapeDtypeStruct((tokens, width), f32),
            jax.ShapeDtypeStruct((nc, LANES), f32),
        ),
        compiler_params=pltpu.CompilerParams(dimension_semantics=("arbitrary",)),
        name="mix",
    )(act, delta, cum, tok, segr, s0, s_in, thr, gate, gains)


def exit_kernel(g_ref, mixed_ref, gate_ref, sq_ref, gain_ref, w_ref, gnorm_ref, *out_refs):
    i = pl.program_id(0)
    rows, width = mixed_ref.shape
    block = lax.rem(g_ref[0] + i, len(out_refs))
    scales = []
    for k in range(rows // CHUNK):
        tot = column(sq_ref[pl.ds(block * (rows // CHUNK) + k, 1), :])
        scales.append(lax.rsqrt(tot / DI + norm_eps))
    scale = jnp.concatenate(scales, axis=0)
    for j in range(width // LANES):
        cs = slice(j * LANES, (j + 1) * LANES)
        g = gate_ref[:, cs]
        gated = mixed_ref[:, cs] * (g * sigmoid(g))
        gnorm_ref[:, cs] = (gated * scale * gain_ref[1:2, cs]).astype(bf16)
    part = dot_nt(gnorm_ref[...], w_ref[...]).astype(bf16)
    for k, out_ref in enumerate(out_refs):

        @pl.when(i == k)
        def _(out_ref=out_ref):
            out_ref[...] = part


def run_exit(group, groups, mixed, gate, sq, gains, weights):
    tokens, width = mixed.shape
    d = weights.shape[0]
    rows = tokens // groups

    def whole(shape, where=0):
        return pl.BlockSpec(
            shape, lambda i, g: (0,) * (len(shape) - 1) + (where,), pipeline_mode=pl.Buffered(1)
        )

    def by_row(w):
        return pl.BlockSpec((rows, w), lambda i, g: (lax.rem(g[0] + i, groups), 0))

    return pl.pallas_call(
        exit_kernel,
        grid_spec=pltpu.PrefetchScalarGridSpec(
            num_scalar_prefetch=1,
            grid=(groups,),
            in_specs=[
                by_row(width),
                by_row(width),
                whole(sq.shape),
                whole(gains.shape),
                whole((d, width), 2),
            ],
            out_specs=(by_row(width),) + (whole((rows, d)),) * groups,
        ),
        out_shape=(jax.ShapeDtypeStruct((tokens, width), bf16),)
        + (jax.ShapeDtypeStruct((rows, d), bf16),) * groups,
        compiler_params=pltpu.CompilerParams(dimension_semantics=("arbitrary",)),
        name="exit",
    )(group, mixed, gate, sq, gains, weights)


def pull_exit_kernel(groups, g_ref, *refs):
    cot_refs, refs = refs[:groups], refs[groups:]
    w_ref, mixed_ref, gate_ref, gnorm_ref, gain_ref, dgn_ref, dot_ref, gw_ref, acc = refs
    i = pl.program_id(0)
    rows, width = mixed_ref.shape
    block = lax.rem(g_ref[0] + groups - i, groups)

    @pl.when(i == 0)
    def _():
        acc[...] = jnp.zeros_like(acc)

    for s, cot_ref in enumerate(cot_refs):

        @pl.when(i == s)
        def _(cot_ref=cot_ref):
            cot = cot_ref[...]
            dgn_ref[...] = dot(cot, w_ref[...])
            acc[...] = acc[...] + lax.dot_general(
                cot, gnorm_ref[...], (((0,), (0,)), ((), ())), preferred_element_type=f32
            )

    part = jnp.zeros((rows, LANES), f32)
    for j in range(width // LANES):
        cs = slice(j * LANES, (j + 1) * LANES)
        g = gate_ref[:, cs]
        gated = mixed_ref[:, cs] * (g * sigmoid(g))
        part = part + dgn_ref[:, cs] * gain_ref[1:2, cs] * gated
    ones = jnp.ones((8, 2 * LANES), bf16)
    for k in range(rows // CHUNK):
        row = dot_nt(ones, jnp.concatenate(split2(part[k * CHUNK : (k + 1) * CHUNK]), axis=1))
        dot_ref[pl.ds(block * (rows // CHUNK) + k, 1), :] = row[0:1]

    @pl.when(i == groups - 1)
    def _():
        gw_ref[...] = acc[...].astype(bf16)


def run_pull_exit(group, groups, cots, weights, mixed, gate, gnorm, gains):
    tokens, width = mixed.shape
    d = weights.shape[0]
    rows = tokens // groups
    nc = tokens // CHUNK

    def whole(shape, where=0):
        return pl.BlockSpec(
            shape, lambda i, g: (0,) * (len(shape) - 1) + (where,), pipeline_mode=pl.Buffered(1)
        )

    def by_row(w):
        return pl.BlockSpec((rows, w), lambda i, g: (lax.rem(g[0] + groups - i, groups), 0))

    return pl.pallas_call(
        functools.partial(pull_exit_kernel, groups),
        grid_spec=pltpu.PrefetchScalarGridSpec(
            num_scalar_prefetch=1,
            grid=(groups,),
            in_specs=[whole((rows, d))] * groups
            + [
                whole((d, width), 2),
                by_row(width),
                by_row(width),
                by_row(width),
                whole(gains.shape),
            ],
            out_specs=(by_row(width), whole((nc, LANES)), whole((d, width))),
            scratch_shapes=[pltpu.VMEM((d, width), f32)],
        ),
        out_shape=(
            jax.ShapeDtypeStruct((tokens, width), f32),
            jax.ShapeDtypeStruct((nc, LANES), f32),
            jax.ShapeDtypeStruct((d, width), bf16),
        ),
        compiler_params=pltpu.CompilerParams(dimension_semantics=("arbitrary",)),
        name="pull_exit",
    )(group, *cots, weights, mixed, gate, gnorm, gains)


def pull_gate_kernel(
    nc,
    mixed_ref,
    gate_ref,
    dgn_ref,
    sq_ref,
    dot_ref,
    gain_ref,
    cum_ref,
    tok_ref,
    act_ref,
    flag_ref,
    dmix_ref,
    dgate_ref,
    g0_ref,
    dinc_ref,
    suf_ref,
    gpart_ref,
    grad,
    total,
    gacc,
):
    i = pl.program_id(0)
    chunk = nc - 1 - i
    width = mixed_ref.shape[1]

    @pl.when(i == 0)
    def _():
        grad[...] = jnp.zeros_like(grad)
        total[...] = jnp.zeros_like(total)
        gacc[...] = jnp.zeros_like(gacc)

    scale = lax.rsqrt(column(sq_ref[pl.ds(chunk, 1), :]) / DI + norm_eps)
    inner = column(dot_ref[pl.ds(chunk, 1), :]) / DI * (scale * scale * scale)
    cum = cum_ref[...]
    last = cum[CHUNK - 1 : CHUNK]
    ramp = jnp.exp(cum) * tok_ref[:, 4:5]
    carry = jnp.exp(last) * flag_ref[pl.ds(chunk, 1), :]
    suf_ref[pl.ds(chunk, 1), :] = jnp.exp(total[0:1]) * flag_ref[pl.ds(2 * nc + chunk, 1), :]
    total[0:1] = total[0:1] + last
    ct = lhs3(*split2(act_ref[...].T))
    for j in range(width // LANES):
        cs = slice(j * LANES, (j + 1) * LANES)
        g = gate_ref[:, cs]
        sg = sigmoid(g)
        gact = g * sg
        mixed = mixed_ref[:, cs]
        gated = mixed * gact
        dgn = dgn_ref[:, cs]
        d_gated = scale * (dgn * gain_ref[1:2, cs]) - gated * inner
        dmix = d_gated * gact
        dmix_ref[:, cs] = dmix
        dgate_ref[:, cs] = (d_gated * mixed * (sg * (1.0 + g * (1.0 - sg)))).astype(bf16)
        gacc[:, cs] = gacc[:, cs] + fold8(dgn * gated * scale)
        g0_ref[0, :, cs] = grad[:, cs]
        dw = dmix * expand(ramp, j)
        grad[:, cs] = grad[:, cs] * expand(carry, j) + dot(ct, rhs3(*split2(dw)))

    @pl.when(i == nc - 1)
    def _():
        dinc_ref[...] = grad[...]
        gpart_ref[...] = gacc[...]


def run_pull_gate(mixed, gate, dgn, sq, dots, gains, cum, tok, act, flags):
    tokens, width = mixed.shape
    nc = tokens // CHUNK

    def whole(shape):
        return pl.BlockSpec(shape, lambda i: (0,) * len(shape))

    def by_row(w, where=0):
        return pl.BlockSpec((CHUNK, w), lambda i: (nc - 1 - i, where))

    return pl.pallas_call(
        functools.partial(pull_gate_kernel, nc),
        grid=(nc,),
        in_specs=[
            by_row(width),
            by_row(width),
            by_row(width),
            whole(sq.shape),
            whole(dots.shape),
            whole(gains.shape),
            by_row(LANES),
            by_row(tok.shape[1]),
            by_row(STATE, (width + STATE) // STATE),
            whole(flags.shape),
        ],
        out_specs=(
            by_row(width),
            by_row(width),
            pl.BlockSpec((1, STATE, width), lambda i: (nc - 1 - i, 0, 0)),
            whole((STATE, width)),
            whole((nc, LANES)),
            whole((8, width)),
        ),
        out_shape=(
            jax.ShapeDtypeStruct((tokens, width), f32),
            jax.ShapeDtypeStruct((tokens, width), bf16),
            jax.ShapeDtypeStruct((nc, STATE, width), f32),
            jax.ShapeDtypeStruct((STATE, width), f32),
            jax.ShapeDtypeStruct((nc, LANES), f32),
            jax.ShapeDtypeStruct((8, width), f32),
        ),
        scratch_shapes=[
            pltpu.VMEM((STATE, width), f32),
            pltpu.VMEM((8, LANES), f32),
            pltpu.VMEM((8, width), f32),
        ],
        compiler_params=pltpu.CompilerParams(dimension_semantics=("arbitrary",)),
        name="pull_gate",
    )(mixed, gate, dgn, sq, dots, gains, cum, tok, act, flags)


def pull_mix_kernel(
    nc,
    u_ref,
    act_ref,
    v_ref,
    vh_ref,
    dmix_ref,
    mixed_ref,
    del_ref,
    cum_ref,
    sig_ref,
    tok_ref,
    segr_ref,
    s0_ref,
    sin_ref,
    fin_ref,
    thr_ref,
    g0_ref,
    gin_ref,
    suf_ref,
    gain_ref,
    par_ref,
    cf_ref,
    dv_ref,
    ddr_ref,
    dvh_ref,
    edge_ref,
    fpart_ref,
    hpart_ref,
    spart_ref,
    du,
    q1,
    q2,
    q3,
    facc,
    hacc,
    sacc,
    send,
):
    i = pl.program_id(0)
    chunk = nc - 1 - i
    width = dmix_ref.shape[1]
    cols = u_ref.shape[1]
    shifted = (q1, q2, q3)

    @pl.when(i == 0)
    def _():
        for q in shifted:
            q[...] = jnp.zeros_like(q)
        facc[...] = jnp.zeros_like(facc)
        hacc[...] = jnp.zeros_like(hacc)
        sacc[...] = jnp.zeros_like(sacc)
        send[...] = fin_ref[...]
        for j in range(width // LANES):
            cs = slice(j * LANES, (j + 1) * LANES)
            send[:, cs] = send[:, cs] + expand(thr_ref[nc : nc + 1, :], j) * sin_ref[:, cs]

    @pl.when(i > 0)
    def _():
        for q in shifted:
            q[CHUNK + 8 : CHUNK + 16] = q[8:16]

    bh, bl = split2(act_ref[:, width : width + STATE])
    ch, cl = split2(act_ref[:, width + STATE :])
    b3 = lhs3(bh, bl)
    scores_t = dot_nt(b3, rhs3_nt(ch, cl))
    cum = cum_ref[...]
    cum_t = cum.T
    r, s = ordered()
    allowed = (tok_ref[:, 5:6] == segr_ref[pl.ds(chunk, 1), :]) & (r <= s)
    bias = jnp.where(allowed, 0.0, NEG)
    delta = del_ref[...]
    last = cum[CHUNK - 1 : CHUNK]
    ramp = jnp.exp(cum) * tok_ref[:, 4:5]
    tail = jnp.exp(last - cum) * tok_ref[:, 3:4]
    thr = thr_ref[pl.ds(chunk, 1), :]
    suf = suf_ref[pl.ds(chunk, 1), :]
    d_scores = jnp.zeros((CHUNK, CHUNK), f32)
    d_b = jnp.zeros((CHUNK, STATE), f32)
    d_c = jnp.zeros((CHUNK, STATE), f32)
    d_delta = jnp.zeros((CHUNK, LANES), f32)
    flow = jnp.zeros((CHUNK, LANES), f32)
    bound = jnp.zeros((8, LANES), f32)
    for j in range(width // LANES):
        cs = slice(j * LANES, (j + 1) * LANES)
        x = act_ref[:, cs]
        dy = dmix_ref[:, cs]
        delta_e = expand(delta, j)
        xd = x * delta_e
        dyh, dyl = split2(dy)
        zero = jnp.zeros_like(dyh)
        keep = left_half(dyh.shape)
        dyh0, dyh1 = jnp.where(keep, dyh, zero), jnp.where(keep, zero, dyh)
        dyl0, dyl1 = jnp.where(keep, dyl, zero), jnp.where(keep, zero, dyl)
        his, los, decays = [], [], []
        for h in (2 * j, 2 * j + 1):
            decay = jnp.exp(cum_t[h : h + 1, :] - cum[:, h : h + 1] + bias)
            hi, lo = split2(scores_t * decay)
            his.append(hi)
            los.append(lo)
            decays.append(decay)
        g_end = g0_ref[0, :, cs] + expand(suf, j) * gin_ref[:, cs]
        st = s0_ref[0, :, cs] + expand(thr, j) * sin_ref[:, cs]
        gh, gl = split2(g_end)
        sh, sl = split2(st)
        tail_e = expand(tail, j)
        dxd = dot(
            jnp.concatenate(his + los + his, axis=1),
            jnp.concatenate([dyh0, dyh1, dyh0, dyh1, dyl0, dyl1], axis=0),
        )
        dxd = dxd + dot(b3, rhs3(gh, gl)) * tail_e
        xdh, xdl = split2(xd)
        d_kernel = dot_nt(
            lhs3(xdh, xdl),
            jnp.concatenate(
                [rhs3_nt(dyh0, dyl0), rhs3_nt(dyh1, dyl1)],
                axis=0,
            ),
        )
        d_scores = d_scores + d_kernel[:, :CHUNK] * decays[0] + d_kernel[:, CHUNK:] * decays[1]
        d_c = d_c + dot_nt(lhs3(*split2(dy * expand(ramp, j))), rhs3_nt(sh, sl))
        d_b = d_b + dot_nt(lhs3(*split2(xd * tail_e)), rhs3_nt(gh, gl))
        skip = gain_ref[0:1, cs]
        yssm = mixed_ref[:, cs] - skip * x
        to_head = head_columns(j)
        to_head2 = jnp.concatenate([to_head, to_head], axis=0)
        d_delta = d_delta + dot(jnp.concatenate(split2(dxd * x), axis=1), to_head2)
        flow = flow + dot(jnp.concatenate(split2(dy * yssm - dxd * xd), axis=1), to_head2)
        met = fold8(g_end * send[:, cs])
        bound = bound + dot(jnp.concatenate(split2(met), axis=1), to_head2)
        send[:, cs] = st
        sacc[:, cs] = sacc[:, cs] + fold8(dy * x)
        u = u_ref[:, cs]
        sg = sigmoid(u)
        du[:, cs] = (dxd * delta_e + skip * dy) * (sg * (1.0 + u * (1.0 - sg)))
    dsh, dsl = split2(d_scores)
    d_b = d_b + dot(lhs3(dsh, dsl), rhs3(ch, cl))
    dth, dtl = split2(d_scores.T)
    d_c = d_c + dot(lhs3(dth, dtl), rhs3(bh, bl))
    for k, value in ((0, d_b), (1, d_c)):
        cs = slice(width + k * STATE, width + (k + 1) * STATE)
        u = u_ref[:, cs]
        sg = sigmoid(u)
        du[:, cs] = value * (sg * (1.0 + u * (1.0 - sg)))
    later = jnp.where(allowed, 1.0, 0.0).astype(bf16)
    later3 = jnp.concatenate([later, later, later], axis=1)
    ends = jnp.sum(bound, axis=0, keepdims=True)
    d_logdec = dot(later3, jnp.concatenate(split3(flow), axis=0)) + ends * tok_ref[:, 3:4]
    d_logdec = d_logdec * tok_ref[:, 2:3]
    ddr = (d_delta + d_logdec * par_ref[1:2, :]) * sig_ref[...]
    ddr_ref[...] = ddr.astype(bf16)
    hacc[0:8] = hacc[0:8] + fold8(ddr)
    hacc[8:16] = hacc[8:16] + fold8(d_logdec * par_ref[1:2, :] * delta)

    masks = [jnp.broadcast_to(tok_ref[:, k : k + 1], (CHUNK, LANES)) for k in (2, 1, 0)]
    for j in range(cols // LANES):
        cs = slice(j * LANES, (j + 1) * LANES)
        d = du[:, cs]
        v = v_ref[:, cs].astype(f32)
        dv = cf_ref[3:4, cs] * d
        facc[32:40, cs] = facc[32:40, cs] + fold8(d)
        facc[24:32, cs] = facc[24:32, cs] + fold8(d * v)
        for n, q in enumerate(shifted, 1):
            q[8 : 8 + CHUNK, cs] = d * masks[n - 1]
            moved = q[8 + n : 8 + n + CHUNK, cs]
            tap = CONV - 1 - n
            dv = dv + cf_ref[tap : tap + 1, cs] * moved
            at = slice(8 * tap, 8 * tap + 8)
            facc[at, cs] = facc[at, cs] + fold8(moved * v)
        dv_ref[:, cs] = dv.astype(bf16)

        @pl.when(i == 0)
        def _(cs=cs, dv=dv):
            edge_ref[:, cs] = dv[CHUNK - 16 :]

    @pl.when(i == nc - 1)
    def _():
        for j in range(cols // LANES):
            cs = slice(j * LANES, (j + 1) * LANES)
            vh = vh_ref[:, cs]
            dvh = jnp.zeros((8, LANES), f32)
            for n, q in enumerate(shifted, 1):
                moved = q[n : n + 8, cs]
                tap = CONV - 1 - n
                dvh = dvh + cf_ref[tap : tap + 1, cs] * moved
                at = slice(8 * tap, 8 * tap + 8)
                facc[at, cs] = facc[at, cs] + moved * vh
            dvh_ref[:, cs] = dvh
        fpart_ref[...] = facc[...]
        hpart_ref[...] = hacc[...]
        spart_ref[...] = sacc[...]


def run_pull_mix(
    u, act, v, vh, dmix, mixed, delta, cum, sig, tok, segr, s0, s_in, fin, thr, g0, g_in, suf,
    gains, par, cf,
):
    tokens, cols = u.shape
    width = dmix.shape[1]
    nc = tokens // CHUNK

    def whole(shape):
        return pl.BlockSpec(
            shape, lambda i: (0,) * len(shape), pipeline_mode=pl.Buffered(1)
        )

    def by_row(w):
        return pl.BlockSpec((CHUNK, w), lambda i: (nc - 1 - i, 0))

    def states():
        return pl.BlockSpec((1, STATE, width), lambda i: (nc - 1 - i, 0, 0))

    def out(shape, dt=f32):
        return jax.ShapeDtypeStruct(shape, dt)

    return pl.pallas_call(
        functools.partial(pull_mix_kernel, nc),
        grid=(nc,),
        in_specs=[
            by_row(cols),
            by_row(cols),
            by_row(cols),
            whole(vh.shape),
            by_row(width),
            by_row(width),
            by_row(LANES),
            by_row(LANES),
            by_row(LANES),
            by_row(tok.shape[1]),
            whole(segr.shape),
            states(),
            whole(s_in.shape),
            whole(fin.shape),
            whole(thr.shape),
            states(),
            whole(g_in.shape),
            whole(suf.shape),
            whole(gains.shape),
            whole(par.shape),
            whole(cf.shape),
        ],
        out_specs=(
            by_row(cols),
            by_row(LANES),
            whole((8, cols)),
            whole((16, cols)),
            whole((40, cols)),
            whole((16, LANES)),
            whole((8, width)),
        ),
        out_shape=(
            out((tokens, cols), bf16),
            out((tokens, LANES), bf16),
            out((8, cols)),
            out((16, cols)),
            out((40, cols)),
            out((16, LANES)),
            out((8, width)),
        ),
        scratch_shapes=[
            pltpu.VMEM((CHUNK, cols), f32),
            pltpu.VMEM((CHUNK + 16, cols), f32),
            pltpu.VMEM((CHUNK + 16, cols), f32),
            pltpu.VMEM((CHUNK + 16, cols), f32),
            pltpu.VMEM((40, cols), f32),
            pltpu.VMEM((16, LANES), f32),
            pltpu.VMEM((8, width), f32),
            pltpu.VMEM((STATE, width), f32),
        ],
        compiler_params=pltpu.CompilerParams(dimension_semantics=("arbitrary",)),
        name="pull_mix",
    )(
        u, act, v, vh, dmix, mixed, delta, cum, sig, tok, segr, s0, s_in, fin, thr, g0, g_in, suf,
        gains, par, cf,
    )


def scatter_kernel(n_dp, n_ctx, n_z, ring, widths, *refs):
    ng = len(widths)
    refs = list(refs)

    def take(n):
        return [refs.pop(0) for _ in range(n)]

    (dn_ref,), parts, (small_ref,) = take(1), take(ng), take(1)
    (dno_ref,), outs, (shared_ref, smalls_ref) = take(1), take(ng - 1), take(2)
    lands, qs, temps, opps, fins = take(ng), take(ng), take(ng), take(ng), take(ng)
    zsh, acc_sh, zland, zsum, sland, ssum, lo, far, near, comb = take(10)
    c_send, c_recv, o_send, o_recv, f_send, f_recv, g_send, g_recv, h_send, h_recv = take(10)
    s_send, s_recv, t_send, t_recv, x_send, x_recv, y_send, y_recv, n_send, n_recv = take(10)
    own = [zsh] + outs

    z, d, c = lax.axis_index("tensor"), lax.axis_index("dp"), lax.axis_index("ctx")
    pos = pick(d, [ring.index(i) for i in range(n_dp)])
    at = [pick(lax.rem(pos + r, n_dp), ring) for r in range(n_dp)]
    nxt, prv = at[1], at[n_dp - 1]
    n_plane = n_dp * n_ctx
    wr = parts[0].shape[0] // n_plane
    rows = dno_ref.shape[0]
    zc = lo.shape[1]
    zr = rows // zc
    step = 16
    mine = d * n_ctx + c

    def remote(src, dst, send, recv, **where):
        return pltpu.make_async_remote_copy(
            src, dst, send, recv, device_id=where, device_id_type=MESH
        )

    def z_at(k):
        return lax.rem(z + k, n_z)

    def c_at(k):
        return lax.rem(c + k, n_ctx)

    peers = [(at[r], c_at(s)) for r in range(n_dp) for s in range(n_ctx) if r or s]
    bar = pltpu.get_barrier_semaphore()
    for dd, cc in peers:
        pl.semaphore_signal(bar, device_id={"dp": dd, "ctx": cc}, device_id_type=MESH)
    for k in range(1, n_z):
        pl.semaphore_signal(bar, device_id={"tensor": z_at(k)}, device_id_type=MESH)
    pl.semaphore_wait(bar, len(peers) + n_z - 1)

    def ctx_copy(g, r, s):
        return remote(
            parts[g].at[pl.ds(pl.multiple_of((at[r] * n_ctx + c_at(s)) * wr, step), wr)],
            lands[g].at[s - 1, r],
            c_send.at[g, s - 1, r],
            c_recv.at[g, s - 1, r],
            ctx=c_at(s),
        )

    cut = [w // 2 // LANES * LANES for w in widths]

    def side(g, h):
        return pl.ds(0, cut[g]) if h == 0 else pl.ds(cut[g], widths[g] - cut[g])

    def opp_copy(g, h):
        return remote(
            qs[g].at[1, :, side(g, h)],
            opps[g].at[:, side(g, h)],
            o_send.at[g, h],
            o_recv.at[g, h],
            dp=nxt if h == 0 else prv,
        )

    def fin_copy(g, way, h):
        return remote(
            qs[g].at[2 * way, :, side(g, h)],
            fins[g].at[way, :, side(g, h)],
            f_send.at[g, way, h],
            f_recv.at[g, way, h],
            dp=nxt if way == 0 else prv,
        )

    def small_copy(i):
        dd, cc = peers[i]
        return remote(small_ref, sland.at[i], s_send.at[i], s_recv.at[i], dp=dd, ctx=cc)

    def small_z(k, src):
        return remote(
            ssum, smalls_ref.at[src], t_send.at[k - 1], t_recv.at[k - 1], tensor=z_at(k)
        )

    def shared_z(k):
        return remote(
            acc_sh.at[z_at(k)], zland.at[k - 1], x_send.at[k - 1], x_recv.at[k - 1], tensor=z_at(k)
        )

    def shared_back(k, src):
        return remote(
            zsum, shared_ref.at[mine, src], y_send.at[k - 1], y_recv.at[k - 1], tensor=z_at(k)
        )

    def shared_dp(r, src):
        return remote(
            shared_ref.at[mine],
            shared_ref.at[src * n_ctx + c],
            g_send.at[r - 1],
            g_recv.at[r - 1],
            dp=at[r],
        )

    def shared_ctx(r, s, src):
        return remote(
            shared_ref.at[at[r] * n_ctx + c],
            shared_ref.at[at[r] * n_ctx + src],
            h_send.at[r, s - 1],
            h_recv.at[r, s - 1],
            ctx=c_at(s),
        )

    outer = (z == 0) | (z == n_z - 1)
    inner = (z > 0) & (z < n_z - 1)
    mate = pick(z, [1, 0, 3, 2])
    far_mate, far_z = n_z - 1 - mate, n_z - 1 - z

    def dn_at(block, k):
        return pl.ds(pl.multiple_of(block * rows + k * zr, step), zr)

    def lo_copy(n, k):
        block = (far_z, far_mate, mate)[n]
        return remote(
            dn_ref.at[dn_at(block, k)], lo.at[n, k], n_send.at[n, k], n_recv.at[n, k], tensor=mate
        )

    def near_copy(k):
        return remote(
            dn_ref.at[dn_at(mate, k)], near.at[k], n_send.at[3, k], n_recv.at[3, k], tensor=mate
        )

    def comb_copy(n, k):
        return remote(
            comb.at[n, k],
            far.at[k],
            n_send.at[4 + n, k],
            n_recv.at[4, k],
            tensor=(far_mate, far_z)[n],
        )

    for g in range(ng):
        for s in range(1, n_ctx):
            for r in range(n_dp):
                ctx_copy(g, r, s).start()

    @pl.when(outer)
    def _():
        for n in range(3):
            for k in range(zc):
                lo_copy(n, k).start()

    @pl.when(inner)
    def _():
        for k in range(zc):
            near_copy(k).start()

    for i in range(len(peers)):
        small_copy(i).start()

    def by_rows(fn):
        def body(i, carry):
            fn(pl.multiple_of(i * step, step))
            return carry

        lax.fori_loop(0, wr // step, body, 0)

    def first(g):
        for s in range(1, n_ctx):
            for r in range(n_dp):
                ctx_copy(g, r, s).wait_recv()

        def body(row):
            for r in range(n_dp):
                base = pl.multiple_of(mine_rows[r] + row, step)
                value = parts[g][pl.ds(base, step)].astype(f32)
                for s in range(n_ctx - 1):
                    value = value + lands[g][s, r, pl.ds(row, step)].astype(f32)
                if r == 0:
                    own[g][pl.ds(row, step)] = value
                else:
                    qs[g][r - 1, pl.ds(row, step)] = value.astype(qs[g].dtype)
                if r == 1:
                    temps[g][pl.ds(row, step), : cut[g]] = value[:, : cut[g]]
                if r == n_dp - 1:
                    temps[g][pl.ds(row, step), cut[g] :] = value[:, cut[g] :]

        by_rows(body)

    mine_rows = [(at[r] * n_ctx + c) * wr for r in range(n_dp)]

    def send_first(g):
        for h in range(2):
            opp_copy(g, h).start()
        fin_copy(g, 0, 1).start()
        fin_copy(g, 1, 0).start()

    def second(g):
        for h in range(2):
            opp_copy(g, h).wait_recv()

        def body(row):
            at_rows = pl.ds(row, step)
            value = temps[g][at_rows] + opps[g][at_rows].astype(f32)
            qs[g][0, at_rows, : cut[g]] = value[:, : cut[g]].astype(qs[g].dtype)
            qs[g][2, at_rows, cut[g] :] = value[:, cut[g] :].astype(qs[g].dtype)

        by_rows(body)

    def send_second(g):
        fin_copy(g, 0, 0).start()
        fin_copy(g, 1, 1).start()

    def third(g):
        for way in range(2):
            for h in range(2):
                fin_copy(g, way, h).wait_recv()

        def body(row):
            at_rows = pl.ds(row, step)
            own[g][at_rows] = (
                own[g][at_rows] + fins[g][0, at_rows].astype(f32) + fins[g][1, at_rows].astype(f32)
            )

        by_rows(body)

    def combine(n, k):
        @pl.when(inner)
        def _():
            lo_copy(n, k).wait_recv()
            block = (far_mate, far_z)[n]
            comb[n, k] = (dn_ref[dn_at(block, k)].astype(f32) + lo[n, k].astype(f32)).astype(bf16)

    def send_combined(n, k):
        @pl.when(inner)
        def _():
            comb_copy(n, k).start()

    first(0)
    first(1)
    send_first(0)
    for i in range(len(peers)):
        small_copy(i).wait_recv()
    total = small_ref[...]
    for i in range(len(peers)):
        total = total + sland[i]
    ssum[...] = total
    smalls_ref[z] = total
    first(2)
    send_first(1)
    for k in range(1, n_z):
        small_z(k, z).start()
    first(3)
    send_first(2)
    second(0)
    send_first(3)
    combine(0, 0)
    send_second(0)
    second(1)
    send_combined(0, 0)
    combine(0, 1)
    send_second(1)
    third(0)
    quarter = wr // n_z
    for k in range(n_z):
        acc_sh[k] = zsh[k * quarter : (k + 1) * quarter]
    second(2)
    send_combined(0, 1)
    for k in range(1, n_z):
        shared_z(k).start()
    combine(1, 0)
    send_second(2)
    for k in range(1, n_z):
        shared_z(k).wait_recv()
    total = acc_sh[z]
    for k in range(1, n_z):
        total = total + zland[k - 1]
    zsum[...] = total
    shared_ref[mine, z] = total
    second(3)
    send_combined(1, 0)
    send_second(3)
    for k in range(1, n_z):
        shared_back(k, z).start()
    combine(1, 1)
    third(1)
    send_combined(1, 1)
    for k in range(1, n_z):
        shared_back(k, z_at(n_z - k)).wait_recv()
    for r in range(1, n_dp):
        shared_dp(r, d).start()
    for s in range(1, n_ctx):
        shared_ctx(0, s, c).start()
    third(2)
    for r in range(1, n_dp):
        shared_dp(r, at[n_dp - r]).wait_recv()
    for r in range(1, n_dp):
        for s in range(1, n_ctx):
            shared_ctx(r, s, c).start()
    third(3)
    for k in range(1, n_z):
        small_z(k, z_at(n_z - k)).wait_recv()
    for k in range(zc):
        at_rows = pl.ds(k * zr, zr)
        dno_ref[at_rows] = dn_ref[dn_at(z, k)].astype(f32)

        @pl.when(outer)
        def _(k=k, at_rows=at_rows):
            near_copy(k).wait_recv()
            dno_ref[at_rows] = dno_ref[at_rows] + near[k].astype(f32)

        @pl.when(inner)
        def _(k=k, at_rows=at_rows):
            lo_copy(2, k).wait_recv()
            dno_ref[at_rows] = dno_ref[at_rows] + lo[2, k].astype(f32)

        comb_copy(0, k).wait_recv()
        dno_ref[at_rows] = dno_ref[at_rows] + far[k].astype(f32)
    for r in range(n_dp):
        for s in range(1, n_ctx):
            shared_ctx(r, s, c_at(n_ctx - s)).wait_recv()

    for g in range(ng):
        for s in range(1, n_ctx):
            for r in range(n_dp):
                ctx_copy(g, r, s).wait_send()
        for h in range(2):
            opp_copy(g, h).wait_send()
            for way in range(2):
                fin_copy(g, way, h).wait_send()

    @pl.when(outer)
    def _():
        for n in range(3):
            for k in range(zc):
                lo_copy(n, k).wait_send()

    @pl.when(inner)
    def _():
        for k in range(zc):
            near_copy(k).wait_send()
            for n in range(2):
                comb_copy(n, k).wait_send()

    for i in range(len(peers)):
        small_copy(i).wait_send()
    for k in range(1, n_z):
        small_z(k, z).wait_send()
        shared_z(k).wait_send()
        shared_back(k, z).wait_send()
    for r in range(1, n_dp):
        shared_dp(r, d).wait_send()
    for r in range(n_dp):
        for s in range(1, n_ctx):
            shared_ctx(r, s, c).wait_send()


def scatter_all(dims, d_normed, parts, small):
    n_dp, n_ctx, n_z, ring = dims
    n_plane = n_dp * n_ctx
    widths = [p.shape[1] for p in parts]
    ng = len(parts)
    wr = parts[0].shape[0] // n_plane
    rows, d = d_normed.shape[0] // n_z, d_normed.shape[1]
    zc = 2
    dma = pltpu.SemaphoreType.DMA
    vmem = pltpu.VMEM
    quarter = wr // n_z

    def out(*shape):
        return jax.ShapeDtypeStruct(shape, f32)

    outs = (
        [out(rows, d)]
        + [out(wr, w) for w in widths[1:]]
        + [out(n_plane, n_z, quarter, widths[0]), out(n_z, *small.shape)]
    )
    scratch = (
        [vmem((n_ctx - 1, n_dp, wr, p.shape[1]), p.dtype) for p in parts]
        + [vmem((3, wr, p.shape[1]), p.dtype) for p in parts]
        + [vmem((wr, w), f32) for w in widths]
        + [vmem((wr, p.shape[1]), p.dtype) for p in parts]
        + [vmem((2, wr, p.shape[1]), p.dtype) for p in parts]
        + [
            vmem((wr, widths[0]), f32),
            vmem((n_z, quarter, widths[0]), f32),
            vmem((n_z - 1, quarter, widths[0]), f32),
            vmem((quarter, widths[0]), f32),
            vmem((n_plane - 1,) + small.shape, f32),
            vmem(small.shape, f32),
            vmem((3, zc, rows // zc, d), bf16),
            vmem((zc, rows // zc, d), bf16),
            vmem((zc, rows // zc, d), bf16),
            vmem((2, zc, rows // zc, d), bf16),
        ]
        + [dma((ng, n_ctx - 1, n_dp))] * 2
        + [dma((ng, 2))] * 2
        + [dma((ng, 2, 2))] * 2
        + [dma((n_dp - 1,))] * 2
        + [dma((n_dp, n_ctx - 1))] * 2
        + [dma((n_plane - 1,))] * 2
        + [dma((n_z - 1,))] * 6
        + [dma((6, zc)), dma((5, zc))]
    )
    return pl.pallas_call(
        functools.partial(scatter_kernel, n_dp, n_ctx, n_z, ring, widths),
        out_shape=tuple(outs),
        in_specs=[pl.BlockSpec(memory_space=pltpu.VMEM)] * (ng + 2),
        out_specs=tuple([pl.BlockSpec(memory_space=pltpu.VMEM)] * len(outs)),
        scratch_shapes=scratch,
        compiler_params=pltpu.CompilerParams(collective_id=3, has_side_effects=True),
        name="scatter_all",
    )(d_normed, *parts, small)


def shift(block, axis, by):
    n = lax.axis_size(axis)
    return lax.ppermute(block, axis, [(i, i + by) for i in range(n) if 0 <= i + by < n])


def turn(block, axis, by):
    n = lax.axis_size(axis)
    return lax.ppermute(block, axis, [(i, (i + by) % n) for i in range(n)])


def adamw(weight, grad, first, second, rate, decay):
    first_new = beta_first * first + (1.0 - beta_first) * grad
    second_new = beta_second * second + (1.0 - beta_second) * grad * grad
    first_hat = first_new / (1.0 - beta_first**STEP)
    second_hat = second_new / (1.0 - beta_second**STEP)
    weight_new = weight - rate * (first_hat / (jnp.sqrt(second_hat) + adam_eps) + decay * weight)
    return (grad, weight_new, first_new, second_new)


def per_lane(row):
    return jnp.repeat(row, HEAD_DIM, axis=-1)


def pad_lanes(a):
    return jnp.pad(a, ((0, 0),) * (a.ndim - 1) + ((0, LANES - a.shape[-1]),))


def state_scan(through, final, axis, reverse):
    n, mine = lax.axis_size(axis), lax.axis_index(axis)
    if n == 2:
        moved = shift(final, axis, -1 if reverse else 1)
        return moved
    finals = lax.all_gather(final, axis)
    rates = lax.all_gather(through, axis)
    acc = jnp.zeros_like(final)
    for k in range(n - 1):
        at = n - 1 - k if reverse else k
        nxt = rates[at] * acc + finals[at]
        acc = jnp.where(at > mine if reverse else at < mine, nxt, acc)
    return acc


def local(
    dims,
    block_in,
    cotangent,
    segments,
    norm_gain,
    inward_weight,
    shared_weight,
    conv_filter,
    head_params,
    gated_gain,
    exit_weight,
    norm_first,
    norm_second,
    entry_first,
    entry_second,
    shared_first,
    shared_second,
    filter_first,
    filter_second,
    head_first,
    head_second,
    gated_first,
    gated_second,
    exit_first,
    exit_second,
):
    group = lax.axis_index("tensor")
    groups = lax.axis_size("tensor")
    per_group = HEADS // groups
    width = DI // groups
    rows = block_in.shape[0]
    tokens = rows * groups
    nc = tokens // CHUNK
    inputs = block_in[:, 0].astype(f32)
    cot = cotangent[:, 0]
    scale_in = lax.rsqrt(jnp.mean(inputs * inputs, axis=-1, keepdims=True) + norm_eps)
    normed_own = (inputs * scale_in * norm_gain).astype(bf16)
    w_own = jnp.concatenate(
        [inward_weight[:, 0], inward_weight[:, 1], exit_weight], axis=1
    ).astype(bf16)

    seg = segments[0]
    prev = shift(seg[-8:], "ctx", 1)
    prev = jnp.where(lax.axis_index("ctx") > 0, prev, -1)
    seg_pad = jnp.concatenate([prev[-3:], seg])
    same = [(seg_pad[k : k + tokens] == seg).astype(f32) for k in range(3)]
    chunks = seg.reshape(nc, CHUNK)
    lasts = chunks[:, -1]
    before = jnp.concatenate([prev[-1:], lasts[:-1]])
    keep = (chunks == lasts[:, None]).astype(f32).reshape(-1)
    inflow = (chunks == before[:, None]).astype(f32).reshape(-1)
    zero = jnp.zeros_like(keep)
    tok = jnp.stack(same + [keep, inflow, seg.astype(f32), zero, zero], axis=1)
    segr = chunks.astype(f32)
    reach = (before == prev[-1]).at[0].set(True)
    flag = jnp.concatenate(
        [
            lasts == before,
            reach,
            lasts == lasts[-1],
            jnp.broadcast_to(lasts[-1] == prev[-1], (nc,)),
        ]
    ).astype(f32)
    flags = jnp.broadcast_to(flag[:, None], (4 * nc, LANES))

    head_own = lax.dynamic_slice_in_dim(head_params, group * per_group, per_group, 1)
    has_prev = jnp.broadcast_to((lax.axis_index("ctx") > 0).astype(f32), (1, LANES))
    par = jnp.concatenate(
        [
            pad_lanes(head_own[0:1]),
            pad_lanes(-jnp.exp(head_own[1:2])),
            jnp.zeros((1, LANES), f32),
            has_prev,
            jnp.zeros((4, LANES), f32),
        ]
    )
    gain_own = lax.dynamic_slice_in_dim(gated_gain, group * width, width)
    gains = jnp.concatenate(
        [per_lane(head_own[2:3]), gain_own[None], jnp.zeros((6, width), f32)]
    )
    cf = jnp.concatenate(
        [
            lax.dynamic_slice_in_dim(conv_filter[:, :DI], group * width, width, 1),
            conv_filter[:, DI:],
        ],
        axis=1,
    )
    cf = jnp.pad(cf, ((0, 3), (0, 0)))
    delta_w = lax.dynamic_slice_in_dim(shared_weight[:, 2 * STATE :], group * per_group, per_group, 1)
    shared_ext = jnp.concatenate(
        [shared_weight[:, : 2 * STATE], pad_lanes(delta_w)], axis=1
    ).astype(bf16)

    shared_bf = jnp.pad(
        shared_weight, ((0, 0), (0, -shared_weight.shape[1] % LANES))
    ).astype(bf16)

    normed, weights, halo = gather_all(dims, normed_own, w_own)

    cot_out = lax.optimization_barrier((cot, halo))[0]
    cots = [cot] + [turn(cot_out, "tensor", k) for k in range(1, groups)]

    gate, v, u, act, delta, cum, sig, s0, fin, thr, vh = run_entry(
        normed, weights, shared_ext, halo, tok, flags, par, cf, width
    )
    through = per_lane(thr[nc : nc + 1, :per_group])
    s_in = state_scan(through, fin, "ctx", False)
    mixed, sq = run_mix(act, delta, cum, tok, segr, s0, s_in, thr, gate, gains)
    sq = all_sum(groups, 1, sq)
    group_at = group.astype(jnp.int32)[None]
    gnorm, *out_parts = run_exit(group_at, groups, mixed, gate, sq, gains, weights)
    total = inputs + out_parts[0].astype(f32)
    for k in range(1, groups):
        total = total + turn(out_parts[k], "tensor", k).astype(f32)
    block_output = total.astype(bf16)[:, None]

    dgn, dots, exit_part = run_pull_exit(
        group_at, groups, cots, weights, mixed, gate, gnorm, gains
    )
    dots = all_sum(groups, 2, dots)
    dmix, d_gate, g0, d_inc, suf, gpart = run_pull_gate(
        mixed, gate, dgn, sq, dots, gains, cum, tok, act, flags
    )
    g_in = state_scan(through, d_inc, "ctx", True)
    d_v, d_raw, d_vh, edge, fpart, hpart, spart = run_pull_mix(
        u, act, v, vh, dmix, mixed, delta, cum, sig, tok, segr, s0, s_in, fin, thr, g0, g_in, suf,
        gains, par, cf,
    )
    from_next = shift(d_vh, "ctx", -1)
    edge = edge.at[8:].add(from_next).astype(bf16)
    d_v = lax.dynamic_update_slice_in_dim(d_v, edge, tokens - 16, 0)

    d_raw = lax.dynamic_update_slice_in_dim(
        jnp.zeros((tokens, LANES), bf16), d_raw[:, :per_group], group * per_group, 1
    )
    d_all = jnp.concatenate([d_gate, d_v, d_raw], axis=1)
    w_all = jnp.concatenate([weights[:, : 2 * width], shared_bf], axis=1)
    back = lax.dot_general(d_all, w_all, NT, preferred_element_type=bf16)
    w_part = lax.dot_general(
        normed, d_all, (((0,), (0,)), ((), ())), preferred_element_type=f32
    )
    norm_part = jnp.sum(w_part * w_all.astype(f32), axis=1) / norm_gain
    shared_part = w_part[:, 2 * width :]
    w_part = w_part.astype(bf16)
    small = jnp.concatenate(
        [
            jnp.sum(gpart, axis=0),
            jnp.sum(fpart[:, :width].reshape(CONV + 1, 8, width), axis=1).reshape(-1),
            pad_lanes(
                jnp.concatenate(
                    [
                        jnp.sum(hpart.reshape(2, 8, LANES), axis=1)[:, :per_group],
                        jnp.sum(spart, axis=0).reshape(1, per_group, HEAD_DIM).sum(-1),
                    ]
                )
            ).reshape(-1),
            jnp.sum(fpart[:, width:].reshape(CONV + 1, 8, 2 * STATE), axis=1).reshape(-1),
            norm_part,
        ]
    )
    n_small = small.shape[0]
    small = jnp.pad(small, (0, -n_small % (8 * LANES))).reshape(-1, LANES)
    d_normed, exit_grad, grad_gate, grad_inner, shared_sum, smalls = scatter_all(
        dims,
        back,
        [shared_part, exit_part, w_part[:, :width], w_part[:, width : 2 * width]],
        small,
    )
    entry_grad = jnp.stack([grad_gate, grad_inner], axis=1)
    shared_grad = shared_sum.reshape(w_part.shape[0], -1)[:, : 2 * STATE + HEADS]
    d_scaled = d_normed * norm_gain
    input_grad = (
        cot.astype(f32)
        + scale_in * d_scaled
        - inputs * scale_in**3 * jnp.mean(d_scaled * inputs, axis=-1, keepdims=True)
    )[:, None]
    smalls = smalls.reshape(groups, -1)
    sizes = [width, (CONV + 1) * width, 3 * LANES, (CONV + 1) * 2 * STATE, norm_gain.shape[0]]
    ends = [sum(sizes[: k + 1]) for k in range(5)]
    gated_grad, f_own, heads, f_shared, norm_grad = (
        smalls[:, e - s : e] for s, e in zip(sizes, ends, strict=True)
    )
    gated_grad = gated_grad.reshape(DI)
    f_own = f_own.reshape(groups, CONV + 1, width).transpose(1, 0, 2).reshape(CONV + 1, DI)
    filter_grad = jnp.concatenate(
        [f_own, jnp.sum(f_shared, axis=0).reshape(CONV + 1, 2 * STATE)], axis=1
    )
    head_grad = (
        heads.reshape(groups, 3, LANES)[:, :, :per_group].transpose(1, 0, 2).reshape(3, HEADS)
    )
    norm_grad = jnp.sum(norm_grad, axis=0)
    return (
        block_output,
        input_grad,
        *adamw(norm_gain, norm_grad, norm_first, norm_second, rate_vector, 0.0),
        *adamw(inward_weight, entry_grad, entry_first, entry_second, rate_matrix, decay_matrix),
        *adamw(shared_weight, shared_grad, shared_first, shared_second, rate_matrix, decay_matrix),
        *adamw(conv_filter, filter_grad, filter_first, filter_second, rate_vector, 0.0),
        *adamw(head_params, head_grad, head_first, head_second, rate_vector, 0.0),
        *adamw(gated_gain, gated_grad, gated_first, gated_second, rate_vector, 0.0),
        *adamw(exit_weight, exit_grad, exit_first, exit_second, rate_matrix, decay_matrix),
    )


def solution(mesh):
    n_dp, n_ctx, n_z = (mesh.shape[a] for a in ("dp", "ctx", "tensor"))
    ring = [0, 1, 3, 2] if n_ctx == 2 and n_dp == 4 else list(range(n_dp))
    dims = (n_dp, n_ctx, n_z, ring)
    token = P(("ctx", "tensor"), "dp", None)
    entry = P(("dp", "ctx"), None, "tensor")
    leave = P(("dp", "ctx"), "tensor")
    rep = P()
    return jax.shard_map(
        functools.partial(local, dims),
        mesh=mesh,
        in_specs=(
            token, token, P("dp", "ctx"), rep, entry, rep, rep, rep, rep, leave,
            rep, rep, entry, entry, rep, rep, rep, rep, rep, rep, rep, rep, leave, leave,
        ),
        out_specs=(token, token)
        + (rep,) * 4 + (entry,) * 4 + (rep,) * 16 + (leave,) * 4,
        check_vma=False,
    )
```

```python
import functools

import jax
import jax.numpy as jnp
from jax import lax
from jax.experimental import pallas as pl
from jax.experimental.pallas import tpu as pltpu
from jax.sharding import PartitionSpec as P


HEADS = 48
HEAD_DIM = 64
STATE = 128
CONV = 4
STEP = 2
DI = 3072
CHUNK = 128
LANES = 128

norm_eps = 1e-05
beta_first = 0.9
beta_second = 0.95
adam_eps = 1e-08
rate_matrix = 0.01
rate_vector = 0.4
decay_matrix = 0.1

MESH = pl.DeviceIdType.MESH
f32 = jnp.float32
bf16 = jnp.bfloat16
NT = (((1,), (1,)), ((), ()))
NEG = -1e30


def pick(index, table):
    out = jnp.int32(table[0])
    for i, v in enumerate(table[1:], 1):
        out = jnp.where(index == i, jnp.int32(v), out)
    return out


def gather_kernel(n_dp, n_ctx, n_z, ring, zc, n_ref, w_ref, seg_ref, nf, wf, halo, pseg, *sems):
    z_send, z_recv, d_send, d_recv, c_send, c_recv, h_sem, l_sem = sems
    z, d, c = lax.axis_index("tensor"), lax.axis_index("dp"), lax.axis_index("ctx")
    pos = pick(d, [ring.index(i) for i in range(n_dp)])
    nxt = pick(lax.rem(pos + 1, n_dp), ring)
    prv = pick(lax.rem(pos + n_dp - 1, n_dp), ring)
    c_next, c_prev = lax.rem(c + 1, n_ctx), lax.rem(c + n_ctx - 1, n_ctx)
    rows, wr = n_ref.shape[0], w_ref.shape[0]
    half, zr = wr // 2, rows // zc
    bar = pltpu.get_barrier_semaphore()

    @pl.when(z > 0)
    def _():
        pl.semaphore_signal(bar, device_id={"tensor": z - 1}, device_id_type=MESH)

    @pl.when(z < n_z - 1)
    def _():
        pl.semaphore_signal(bar, device_id={"tensor": z + 1}, device_id_type=MESH)

    pl.semaphore_signal(bar, device_id={"dp": nxt}, device_id_type=MESH)
    pl.semaphore_signal(bar, device_id={"dp": prv}, device_id_type=MESH)
    pl.semaphore_signal(bar, device_id={"ctx": c_prev}, device_id_type=MESH)
    if n_ctx > 2:
        pl.semaphore_signal(bar, device_id={"ctx": c_next}, device_id_type=MESH)
    extra = 3 if n_ctx == 2 else 4

    @pl.when((z > 0) & (z < n_z - 1))
    def _():
        pl.semaphore_wait(bar, extra + 2)

    @pl.when((z == 0) | (z == n_z - 1))
    def _():
        pl.semaphore_wait(bar, extra + 1)

    def zcopy(src, k, to, first, way):
        here = nf.at[pl.ds(src * rows + k * zr, zr)]
        return pltpu.make_async_remote_copy(
            n_ref.at[pl.ds(k * zr, zr)] if first else here,
            here,
            z_send.at[way, src, k],
            z_recv.at[src, k],
            device_id={"tensor": to},
            device_id_type=MESH,
        )

    def wpart(cc, dd, h):
        return wf.at[pl.ds((dd * n_ctx + cc) * wr + h * half, half)]

    def dcopy(sp, h, first):
        here = wpart(c, pick(sp, ring), h)
        return pltpu.make_async_remote_copy(
            w_ref.at[pl.ds(h * half, half)] if first else here,
            here,
            d_send.at[sp, h],
            d_recv.at[sp, h],
            device_id={"dp": nxt if h == 0 else prv},
            device_id_type=MESH,
        )

    def ccopy(cc, dd, h, first):
        here = wpart(cc, dd, h)
        return pltpu.make_async_remote_copy(
            w_ref.at[pl.ds(h * half, half)] if first else here,
            here,
            c_send.at[cc, dd, h],
            c_recv.at[cc, dd, h],
            device_id={"ctx": c_next},
            device_id_type=MESH,
        )

    def ring_pos(dist, h):
        return lax.rem(pos + (n_dp - dist if h == 0 else dist), n_dp)

    for k in range(zc):

        @pl.when(z < n_z - 1)
        def _(k=k):
            zcopy(z, k, z + 1, True, 0).start()

        @pl.when(z > 0)
        def _(k=k):
            zcopy(z, k, z - 1, True, 1).start()

        if k == 0:
            for h in range(2):
                dcopy(pos, h, True).start()
            for h in range(2):
                ccopy(c, d, h, True).start()
            own_w = pltpu.make_async_copy(
                w_ref, wf.at[pl.ds((d * n_ctx + c) * wr, wr)], l_sem.at[0]
            )
            own_n = pltpu.make_async_copy(n_ref, nf.at[pl.ds(z * rows, rows)], l_sem.at[1])
            own_w.start()
            own_n.start()
    for dist in range(1, max(n_z, n_dp)):
        for k in range(zc):
            if dist < n_z:

                @pl.when(z >= dist)
                def _(k=k, dist=dist):
                    zcopy(z - dist, k, z, False, 0).wait_recv()

                    @pl.when(z < n_z - 1)
                    def _():
                        zcopy(z - dist, k, z + 1, False, 0).start()

                @pl.when(z + dist < n_z)
                def _(k=k, dist=dist):
                    zcopy(z + dist, k, z, False, 1).wait_recv()

                    @pl.when(z > 0)
                    def _():
                        zcopy(z + dist, k, z - 1, False, 1).start()

            if k == 0 and dist < n_dp:
                for h in range(2):
                    sp = ring_pos(dist, h)
                    dcopy(sp, h, False).wait_recv()
                    if dist < n_dp - 1:
                        dcopy(sp, h, False).start()
                    ccopy(c, pick(sp, ring), h, False).start()
    own_n.wait()
    own_w.wait()
    edge = pltpu.make_async_remote_copy(
        nf.at[pl.ds(n_z * rows - halo.shape[0], halo.shape[0])],
        halo,
        h_sem.at[0],
        h_sem.at[1],
        device_id={"ctx": c_next},
        device_id_type=MESH,
    )
    edge.start()
    ids = pltpu.make_async_remote_copy(
        seg_ref, pseg, h_sem.at[2], h_sem.at[3], device_id={"ctx": c_next}, device_id_type=MESH
    )
    ids.start()
    for step in range(1, n_ctx):
        cc = lax.rem(c + n_ctx - step, n_ctx)
        for dist in range(n_dp):
            for h in range(2):
                dd = pick(ring_pos(dist, h), ring)
                ccopy(cc, dd, h, False).wait_recv()
                if step < n_ctx - 1:
                    ccopy(cc, dd, h, False).start()
    edge.wait()
    ids.wait()
    for k in range(zc):
        for dist in range(n_z):

            @pl.when((z >= dist) & (z < n_z - 1))
            def _(k=k, dist=dist):
                zcopy(z - dist, k, z + 1, dist == 0, 0).wait_send()

            @pl.when((z + dist < n_z) & (z > 0))
            def _(k=k, dist=dist):
                zcopy(z + dist, k, z - 1, dist == 0, 1).wait_send()

    for dist in range(n_dp):
        for h in range(2):
            sp = ring_pos(dist, h)
            if dist < n_dp - 1:
                dcopy(sp, h, dist == 0).wait_send()
            for step in range(n_ctx - 1):
                cc = lax.rem(c + n_ctx - step, n_ctx)
                ccopy(cc, pick(sp, ring), h, dist == 0 and step == 0).wait_send()


def gather_all(dims, normed, weights, seg):
    n_dp, n_ctx, n_z, ring = dims
    rows, width = normed.shape
    wr, wc = weights.shape
    zc = 2
    dma = pltpu.SemaphoreType.DMA
    return pl.pallas_call(
        functools.partial(gather_kernel, n_dp, n_ctx, n_z, ring, zc),
        out_shape=(
            jax.ShapeDtypeStruct((rows * n_z, width), normed.dtype),
            jax.ShapeDtypeStruct((wr * n_dp * n_ctx, wc), weights.dtype),
            jax.ShapeDtypeStruct((16, width), normed.dtype),
            jax.ShapeDtypeStruct(seg.shape, seg.dtype),
        ),
        in_specs=[pl.BlockSpec(memory_space=pltpu.VMEM)] * 3,
        out_specs=tuple([pl.BlockSpec(memory_space=pl.ANY)] * 4),
        scratch_shapes=[
            dma((2, n_z, zc)),
            dma((n_z, zc)),
            dma((n_dp, 2)),
            dma((n_dp, 2)),
            dma((n_ctx, n_dp, 2)),
            dma((n_ctx, n_dp, 2)),
            dma((4,)),
            dma((2,)),
        ],
        compiler_params=pltpu.CompilerParams(collective_id=0, has_side_effects=True),
        name="gather_all",
    )(normed, weights, seg)


def all_sum_kernel(n_z, x_ref, y_ref, ox_ref, oy_ref, land, send, recv):
    z = lax.axis_index("tensor")
    bar = pltpu.get_barrier_semaphore()
    for k in range(1, n_z):
        pl.semaphore_signal(
            bar, device_id={"tensor": lax.rem(z + k, n_z)}, device_id_type=MESH
        )
    pl.semaphore_wait(bar, n_z - 1)
    copies = []
    for n, ref in enumerate((x_ref, y_ref)):
        for k in range(1, n_z):
            copy = pltpu.make_async_remote_copy(
                ref,
                land.at[n, k - 1],
                send.at[n, k - 1],
                recv.at[n, k - 1],
                device_id={"tensor": lax.rem(z + k, n_z)},
                device_id_type=MESH,
            )
            copy.start()
            copies.append(copy)
    for copy in copies:
        copy.wait()
    for n, (ref, out) in enumerate(((x_ref, ox_ref), (y_ref, oy_ref))):
        total = ref[...]
        for k in range(1, n_z):
            total = total + land[n, k - 1]
        out[...] = total


def all_sum(n_z, collective_id, x, y):
    return pl.pallas_call(
        functools.partial(all_sum_kernel, n_z),
        out_shape=(jax.ShapeDtypeStruct(x.shape, x.dtype),) * 2,
        in_specs=[pl.BlockSpec(memory_space=pltpu.VMEM)] * 2,
        out_specs=(pl.BlockSpec(memory_space=pltpu.VMEM),) * 2,
        scratch_shapes=[
            pltpu.VMEM((2, n_z - 1) + x.shape, x.dtype),
            pltpu.SemaphoreType.DMA((2, n_z - 1)),
            pltpu.SemaphoreType.DMA((2, n_z - 1)),
        ],
        compiler_params=pltpu.CompilerParams(collective_id=collective_id, has_side_effects=True),
        name="all_sum",
    )(x, y)


def split2(a):
    hi = a.astype(bf16)
    return hi, (a - hi.astype(f32)).astype(bf16)


def split3(a):
    hi = a.astype(bf16)
    rest = a - hi.astype(f32)
    mid = rest.astype(bf16)
    return hi, mid, (rest - mid.astype(f32)).astype(bf16)


def dot(a, b):
    return jnp.dot(a, b, preferred_element_type=f32)


def dot_nt(a, b):
    return lax.dot_general(a, b, NT, preferred_element_type=f32)


def lhs3(hi, lo):
    return jnp.concatenate([hi, lo, hi], axis=1)


def rhs3(hi, lo):
    return jnp.concatenate([hi, hi, lo], axis=0)


def rhs3_nt(hi, lo):
    return jnp.concatenate([hi, hi, lo], axis=1)


def left_half(shape):
    return lax.broadcasted_iota(jnp.int32, shape, 1) < HEAD_DIM


def expand(v, j):
    shape = (v.shape[0], LANES)
    return jnp.where(
        left_half(shape),
        jnp.broadcast_to(v[:, 2 * j : 2 * j + 1], shape),
        jnp.broadcast_to(v[:, 2 * j + 1 : 2 * j + 2], shape),
    )


def column(row):
    return jnp.broadcast_to(row, (LANES, LANES)).T


def ordered(length=CHUNK):
    r = lax.broadcasted_iota(jnp.int32, (length, length), 0)
    c = lax.broadcasted_iota(jnp.int32, (length, length), 1)
    return r, c


def fold8(a):
    out = a[0:8]
    for k in range(8, a.shape[0], 8):
        out = out + a[k : k + 8]
    return out


def head_columns(j):
    r, c = ordered(LANES)
    return jnp.where(c == 2 * j + jnp.where(r < HEAD_DIM, 0, 1), 1.0, 0.0).astype(bf16)


def sigmoid(x):
    return 1.0 / (1.0 + jnp.exp(-x))


SEG, BACK1, BACK2, BACK3, BEFORE, LAST, KEEPS, REACHES, STAYS, THROUGH = range(10)


class Masks:
    def __init__(self, rows_ref, nc, chunk):
        self.rows_ref, self.nc, self.chunk = rows_ref, nc, chunk
        self.seg = column(self.row(SEG))

    def row(self, kind):
        return self.rows_ref[pl.ds(kind * self.nc + self.chunk, 1), :]

    def same(self, kind):
        return jnp.where(self.seg == column(self.row(kind)), 1.0, 0.0)


def prep_kernel(x_ref, gain_ref, w_ref, we_ref, ws_ref, n_out, w_out, ws_out, buf, sem):
    def plane(which):
        return pltpu.make_async_copy(w_ref.at[:, which, :], buf.at[which], sem.at[which])

    for which in range(2):
        plane(which).start()
    x = x_ref[...].astype(f32)
    scale = lax.rsqrt(jnp.mean(x * x, axis=-1, keepdims=True) + norm_eps)
    n_out[...] = (x * scale * gain_ref[...]).astype(bf16)
    width = we_ref.shape[1]
    w_out[:, 2 * width :] = we_ref[...].astype(bf16)
    n = ws_ref.shape[0]
    ws_out[:n] = ws_ref[...].astype(bf16)
    ws_out[n:] = jnp.zeros((ws_out.shape[0] - n, ws_out.shape[1]), bf16)
    for which in range(2):
        plane(which).wait()
        w_out[:, which * width : (which + 1) * width] = buf[which].astype(bf16)


def run_prep(x, gain, w, we, ws):
    rows, width = we.shape
    n = ws.shape[0]
    return pl.pallas_call(
        prep_kernel,
        out_shape=(
            jax.ShapeDtypeStruct(x.shape, bf16),
            jax.ShapeDtypeStruct((rows, 3 * width), bf16),
            jax.ShapeDtypeStruct((n + -n % LANES, ws.shape[1]), bf16),
        ),
        in_specs=[pl.BlockSpec(memory_space=pltpu.VMEM)] * 2
        + [pl.BlockSpec(memory_space=pl.ANY)]
        + [pl.BlockSpec(memory_space=pltpu.VMEM)] * 2,
        scratch_shapes=[pltpu.VMEM((2, rows, width), f32), pltpu.SemaphoreType.DMA((2,))],
        name="prep",
    )(x, gain, w, we, ws)


def entry_kernel(
    nc,
    per_group,
    at_ref,
    n_ref,
    w_ref,
    ws_ref,
    halo_ref,
    seg_ref,
    pseg_ref,
    hp_ref,
    gg_ref,
    cfa_ref,
    cfb_ref,
    gate_ref,
    v_ref,
    u_ref,
    act_ref,
    del_ref,
    cum_ref,
    sig_ref,
    s0_ref,
    fin_ref,
    thr_ref,
    vh_ref,
    rows_ref,
    par_ref,
    gains_ref,
    vbuf,
    state,
    total,
):
    i = pl.program_id(0)
    rows = n_ref.shape[0]
    width = gate_ref.shape[1]
    cols = v_ref.shape[1]
    group, has_prev = at_ref[0], at_ref[1]
    lane = lax.broadcasted_iota(jnp.int32, (8, LANES), 1)

    def to_own(a):
        moved = pltpu.roll(a, lax.rem(LANES - group * per_group, LANES), 1)
        return jnp.where(lax.broadcasted_iota(jnp.int32, a.shape, 1) < per_group, moved, 0.0)

    @pl.when(i == 0)
    def _():
        hv = jnp.concatenate(
            [dot(halo_ref[...], w_ref[:, width:]), dot_nt(halo_ref[...], ws_ref[: 2 * STATE])],
            axis=1,
        )
        hv = jnp.where(has_prev > 0, hv.astype(bf16).astype(f32), 0.0)
        vbuf[0:8] = hv[8:16]
        vh_ref[...] = hv[8:16]
        state[...] = jnp.zeros_like(state)
        total[...] = jnp.zeros_like(total)

        seg = seg_ref[...].astype(f32)
        prev = jnp.where(has_prev > 0, pseg_ref[...].astype(f32), -1.0)
        ahead = jnp.concatenate([prev[nc - 1 : nc], seg[: nc - 1]], axis=0)
        ends = jnp.broadcast_to(seg[:, LANES - 1 :], (nc, LANES))
        starts = jnp.broadcast_to(ahead[:, LANES - 1 :], (nc, LANES))
        first = jnp.broadcast_to(prev[nc - 1 : nc, LANES - 1 :], (nc, LANES))
        final = jnp.broadcast_to(seg[nc - 1 : nc, LANES - 1 :], (nc, LANES))
        top = lax.broadcasted_iota(jnp.int32, (nc, LANES), 0) == 0
        place = lax.broadcasted_iota(jnp.int32, (nc, LANES), 1)
        kinds = [seg]
        for k in range(1, CONV):
            kinds.append(jnp.where(place < k, pltpu.roll(ahead, k, 1), pltpu.roll(seg, k, 1)))
        kinds += [
            starts,
            ends,
            jnp.where(ends == starts, 1.0, 0.0),
            jnp.where(top | (starts == first), 1.0, 0.0),
            jnp.where(ends == final, 1.0, 0.0),
            jnp.where(final == first, 1.0, 0.0),
        ]
        for k, kind in enumerate(kinds):
            rows_ref[k * nc : (k + 1) * nc] = kind
        own = to_own(hp_ref[...])
        par = jnp.where(
            lax.broadcasted_iota(jnp.int32, (8, LANES), 0) == 1,
            jnp.where(lane < per_group, -jnp.exp(own), 0.0),
            own,
        )
        par_ref[...] = par
        for j in range(width // LANES):
            cs = slice(j * LANES, (j + 1) * LANES)
            gains_ref[0:1, cs] = expand(par[2:3], j)
            gains_ref[1:2, cs] = gg_ref[pl.ds(group * (width // LANES) + j, 1), :]

    @pl.when(i > 0)
    def _():
        vbuf[0:8] = vbuf[rows : rows + 8]

    n = n_ref[...]
    gate_ref[...] = dot(n, w_ref[:, :width])
    vi = dot(n, w_ref[:, width:]).astype(bf16)
    v_ref[:, :width] = vi
    vbuf[8 : rows + 8, :width] = vi.astype(f32)
    sh = dot_nt(n, ws_ref[...])
    vb = sh[:, : 2 * STATE].astype(bf16)
    v_ref[:, width:] = vb
    vbuf[8 : rows + 8, width:] = vb.astype(f32)
    raw = to_own(sh[:, 2 * STATE :]) + par_ref[0:1, :]
    delta = jnp.maximum(raw, 0.0) + jnp.log1p(jnp.exp(-jnp.abs(raw)))
    del_ref[...] = delta
    sig_ref[...] = sigmoid(raw)
    logdec = par_ref[1:2, :] * delta

    chunks = [Masks(rows_ref, nc, i * (rows // CHUNK) + k) for k in range(rows // CHUNK)]
    masks = [
        jnp.concatenate([m.same(kind) for m in chunks], axis=0) for kind in (BACK3, BACK2, BACK1)
    ]
    for j in range(cols // LANES):
        cs = slice(j * LANES, (j + 1) * LANES)
        cf = cfa_ref[:, cs] if j < width // LANES else cfb_ref[:, j * LANES - width :][:, :LANES]
        u = cf[4:5] + cf[3:4] * vbuf[8 : 8 + rows, cs]
        for k in range(3):
            u = u + cf[k : k + 1] * vbuf[5 + k : 5 + k + rows, cs] * masks[k]
        u_ref[:, cs] = u
        act_ref[:, cs] = u * sigmoid(u)

    r, c = ordered()
    tri = jnp.where(r >= c, 1.0, 0.0).astype(bf16)
    tri3 = jnp.concatenate([tri, tri, tri], axis=1)
    for k in range(rows // CHUNK):
        ts = slice(k * CHUNK, (k + 1) * CHUNK)
        chunk = i * (rows // CHUNK) + k
        cum = dot(tri3, jnp.concatenate(split3(logdec[ts]), axis=0))
        cum_ref[ts] = cum
        last = cum[CHUNK - 1 : CHUNK]
        weight = jnp.exp(last - cum) * chunks[k].same(LAST) * delta[ts]
        carry = jnp.exp(last) * chunks[k].row(KEEPS)
        thr_ref[pl.ds(chunk, 1), :] = jnp.exp(total[0:1]) * chunks[k].row(REACHES)
        total[0:1] = total[0:1] + last
        bt = lhs3(*split2(act_ref[ts, width : width + STATE].T))
        for j in range(width // LANES):
            cs = slice(j * LANES, (j + 1) * LANES)
            s0_ref[k, :, cs] = state[:, cs]
            xw = act_ref[ts, cs] * expand(weight, j)
            state[:, cs] = state[:, cs] * expand(carry, j) + dot(bt, rhs3(*split2(xw)))

    @pl.when(i == pl.num_programs(0) - 1)
    def _():
        thr_ref[nc : nc + 8, :] = jnp.broadcast_to(
            jnp.exp(total[0:1]) * rows_ref[THROUGH * nc : THROUGH * nc + 1, :], (8, LANES)
        )
        fin_ref[...] = state[...]


def run_entry(at, per_group, normed, weights, ws, halo, seg, pseg, hp, gg, conv_filter):
    tokens, d = normed.shape
    rows = 256
    nc = tokens // CHUNK
    width = weights.shape[1] // 3
    cols = width + 2 * STATE
    one = pl.Buffered(1)

    def whole(shape):
        return pl.BlockSpec(shape, lambda i, at: (0,) * len(shape), pipeline_mode=one)

    def by_row(w):
        return pl.BlockSpec((rows, w), lambda i, at: (i, 0))

    def out(shape, dt=f32):
        return jax.ShapeDtypeStruct(shape, dt)

    taps = conv_filter.shape[0]
    return pl.pallas_call(
        functools.partial(entry_kernel, nc, per_group),
        grid_spec=pltpu.PrefetchScalarGridSpec(
            num_scalar_prefetch=1,
            grid=(tokens // rows,),
            in_specs=[
                by_row(d),
                whole((d, 2 * width)),
                whole(ws.shape),
                whole(halo.shape),
                whole(seg.shape),
                whole(pseg.shape),
                whole(hp.shape),
                whole(gg.shape),
                pl.BlockSpec((taps, width), lambda i, at: (0, at[0])),
                pl.BlockSpec((taps, 2 * STATE), lambda i, at: (0, DI // (2 * STATE))),
            ],
            out_specs=(
                by_row(width),
                by_row(cols),
                by_row(cols),
                by_row(cols),
                by_row(LANES),
                by_row(LANES),
                by_row(LANES),
                pl.BlockSpec((rows // CHUNK, STATE, width), lambda i, at: (i, 0, 0)),
                whole((STATE, width)),
                whole((nc + 8, LANES)),
                whole((8, cols)),
                whole((10 * nc, LANES)),
                whole((8, LANES)),
                whole((8, width)),
            ),
            scratch_shapes=[
                pltpu.VMEM((rows + 8, cols), f32),
                pltpu.VMEM((STATE, width), f32),
                pltpu.VMEM((8, LANES), f32),
            ],
        ),
        out_shape=(
            out((tokens, width)),
            out((tokens, cols), bf16),
            out((tokens, cols)),
            out((tokens, cols)),
            out((tokens, LANES)),
            out((tokens, LANES)),
            out((tokens, LANES)),
            out((nc, STATE, width)),
            out((STATE, width)),
            out((nc + 8, LANES)),
            out((8, cols)),
            out((10 * nc, LANES)),
            out((8, LANES)),
            out((8, width)),
        ),
        compiler_params=pltpu.CompilerParams(dimension_semantics=("arbitrary",)),
        name="entry",
    )(at, normed, weights, ws, halo, seg, pseg, hp, gg, conv_filter, conv_filter)


def mix_kernel(
    act_ref,
    del_ref,
    cum_ref,
    rows_ref,
    s0_ref,
    sin_ref,
    thr_ref,
    gate_ref,
    gain_ref,
    mixed_ref,
    sq_ref,
):
    chunk = pl.program_id(0)
    masks = Masks(rows_ref, rows_ref.shape[0] // 10, chunk)
    width = gate_ref.shape[1]
    b = act_ref[:, width : width + STATE]
    c = act_ref[:, width + STATE :]
    bh, bl = split2(b)
    ch, cl = split2(c)
    c3 = lhs3(ch, cl)
    scores = dot_nt(c3, rhs3_nt(bh, bl))
    cum = cum_ref[...]
    cum_t = cum.T
    r, s = ordered()
    bias = jnp.where((masks.seg == masks.row(SEG)) & (r >= s), 0.0, NEG)
    delta = del_ref[...]
    ramp = jnp.exp(cum) * masks.same(BEFORE)
    thr = thr_ref[pl.ds(chunk, 1), :]
    squares = jnp.zeros((CHUNK, LANES), f32)
    for j in range(width // LANES):
        cs = slice(j * LANES, (j + 1) * LANES)
        x = act_ref[:, cs]
        his, los = [], []
        for h in (2 * j, 2 * j + 1):
            decay = jnp.exp(cum[:, h : h + 1] - cum_t[h : h + 1, :] + bias)
            hi, lo = split2(scores * decay)
            his.append(hi)
            los.append(lo)
        xh, xl = split2(x * expand(delta, j))
        zero = jnp.zeros_like(xh)
        keep = left_half(xh.shape)
        xh0, xh1 = jnp.where(keep, xh, zero), jnp.where(keep, zero, xh)
        xl0, xl1 = jnp.where(keep, xl, zero), jnp.where(keep, zero, xl)
        y = dot(
            jnp.concatenate(his + los + his, axis=1),
            jnp.concatenate([xh0, xh1, xh0, xh1, xl0, xl1], axis=0),
        )
        st = s0_ref[0, :, cs] + expand(thr, j) * sin_ref[:, cs]
        y = y + dot(c3, rhs3(*split2(st))) * expand(ramp, j)
        mixed = y + gain_ref[0:1, cs] * x
        mixed_ref[:, cs] = mixed
        g = gate_ref[:, cs]
        gated = mixed * (g * sigmoid(g))
        squares = squares + gated * gated
    ones = jnp.ones((8, 2 * LANES), bf16)
    sq_ref[pl.ds(chunk, 1), :] = dot_nt(ones, jnp.concatenate(split2(squares), axis=1))[0:1]


def run_mix(act, delta, cum, table, s0, s_in, thr, gate, gains):
    tokens, cols = act.shape
    width = gate.shape[1]
    nc = tokens // CHUNK

    def whole(shape):
        return pl.BlockSpec(shape, lambda i: (0,) * len(shape))

    def by_row(w):
        return pl.BlockSpec((CHUNK, w), lambda i: (i, 0))

    return pl.pallas_call(
        mix_kernel,
        grid=(nc,),
        in_specs=[
            by_row(cols),
            by_row(LANES),
            by_row(LANES),
            whole(table.shape),
            pl.BlockSpec((1, STATE, width), lambda i: (i, 0, 0)),
            whole(s_in.shape),
            whole(thr.shape),
            by_row(width),
            whole(gains.shape),
        ],
        out_specs=(by_row(width), whole((nc, LANES))),
        out_shape=(
            jax.ShapeDtypeStruct((tokens, width), f32),
            jax.ShapeDtypeStruct((nc, LANES), f32),
        ),
        compiler_params=pltpu.CompilerParams(dimension_semantics=("arbitrary",)),
        name="mix",
    )(act, delta, cum, table, s0, s_in, thr, gate, gains)


def exit_kernel(g_ref, mixed_ref, gate_ref, sq_ref, gain_ref, w_ref, gnorm_ref, *out_refs):
    i = pl.program_id(0)
    rows, width = mixed_ref.shape
    block = lax.rem(g_ref[0] + i, len(out_refs))
    scales = []
    for k in range(rows // CHUNK):
        tot = column(sq_ref[pl.ds(block * (rows // CHUNK) + k, 1), :])
        scales.append(lax.rsqrt(tot / DI + norm_eps))
    scale = jnp.concatenate(scales, axis=0)
    for j in range(width // LANES):
        cs = slice(j * LANES, (j + 1) * LANES)
        g = gate_ref[:, cs]
        gated = mixed_ref[:, cs] * (g * sigmoid(g))
        gnorm_ref[:, cs] = (gated * scale * gain_ref[1:2, cs]).astype(bf16)
    part = dot_nt(gnorm_ref[...], w_ref[...]).astype(bf16)
    for k, out_ref in enumerate(out_refs):

        @pl.when(i == k)
        def _(out_ref=out_ref):
            out_ref[...] = part


def run_exit(group, groups, mixed, gate, sq, gains, weights):
    tokens, width = mixed.shape
    d = weights.shape[0]
    rows = tokens // groups

    def whole(shape, where=0):
        return pl.BlockSpec(
            shape, lambda i, g: (0,) * (len(shape) - 1) + (where,), pipeline_mode=pl.Buffered(1)
        )

    def by_row(w):
        return pl.BlockSpec((rows, w), lambda i, g: (lax.rem(g[0] + i, groups), 0))

    return pl.pallas_call(
        exit_kernel,
        grid_spec=pltpu.PrefetchScalarGridSpec(
            num_scalar_prefetch=1,
            grid=(groups,),
            in_specs=[
                by_row(width),
                by_row(width),
                whole(sq.shape),
                whole(gains.shape),
                whole((d, width), 2),
            ],
            out_specs=(by_row(width),) + (whole((rows, d)),) * groups,
        ),
        out_shape=(jax.ShapeDtypeStruct((tokens, width), bf16),)
        + (jax.ShapeDtypeStruct((rows, d), bf16),) * groups,
        compiler_params=pltpu.CompilerParams(dimension_semantics=("arbitrary",)),
        name="exit",
    )(group, mixed, gate, sq, gains, weights)


def from_line(refs, groups, group, step):
    pairs = [(refs[0], step == 0)]
    for k in range(1, groups):
        pairs.append((refs[k], (step == k) & (group >= k)))
        pairs.append((refs[groups - 1 + k], (step == groups - k) & (group < groups - k)))
    return pairs


def pull_exit_kernel(groups, g_ref, *refs):
    n_cot = 2 * groups - 1
    cot_refs, refs = refs[:n_cot], refs[n_cot:]
    w_ref, mixed_ref, gate_ref, gain_ref, dgn_ref, dot_ref = refs
    i = pl.program_id(0)
    rows, width = mixed_ref.shape
    block = lax.rem(g_ref[0] + groups - i, groups)
    for cot_ref, here in from_line(cot_refs, groups, g_ref[0], i):

        @pl.when(here)
        def _(cot_ref=cot_ref):
            dgn_ref[...] = dot(cot_ref[...], w_ref[...])

    part = jnp.zeros((rows, LANES), f32)
    for j in range(width // LANES):
        cs = slice(j * LANES, (j + 1) * LANES)
        g = gate_ref[:, cs]
        gated = mixed_ref[:, cs] * (g * sigmoid(g))
        part = part + dgn_ref[:, cs] * gain_ref[1:2, cs] * gated
    ones = jnp.ones((8, 2 * LANES), bf16)
    for k in range(rows // CHUNK):
        row = dot_nt(ones, jnp.concatenate(split2(part[k * CHUNK : (k + 1) * CHUNK]), axis=1))
        dot_ref[pl.ds(block * (rows // CHUNK) + k, 1), :] = row[0:1]


def exit_grad_kernel(groups, g_ref, *refs):
    n_cot = 2 * groups - 1
    cot_refs, (gnorm_ref, gw_ref, acc) = refs[:n_cot], refs[n_cot:]
    i = pl.program_id(0)

    @pl.when(i == 0)
    def _():
        acc[...] = jnp.zeros_like(acc)

    for cot_ref, here in from_line(cot_refs, groups, g_ref[0], i):

        @pl.when(here)
        def _(cot_ref=cot_ref):
            acc[...] = acc[...] + lax.dot_general(
                cot_ref[...], gnorm_ref[...], (((0,), (0,)), ((), ())), preferred_element_type=f32
            )

    @pl.when(i == groups - 1)
    def _():
        gw_ref[...] = acc[...].astype(bf16)


def run_exit_grad(group, groups, cots, gnorm):
    _, width = gnorm.shape
    rows, d = cots[0].shape

    def whole(shape):
        return pl.BlockSpec(
            shape, lambda i, g: (0,) * len(shape), pipeline_mode=pl.Buffered(1)
        )

    return pl.pallas_call(
        functools.partial(exit_grad_kernel, groups),
        grid_spec=pltpu.PrefetchScalarGridSpec(
            num_scalar_prefetch=1,
            grid=(groups,),
            in_specs=[whole((rows, d))] * len(cots)
            + [pl.BlockSpec((rows, width), lambda i, g: (lax.rem(g[0] + groups - i, groups), 0))],
            out_specs=whole((d, width)),
            scratch_shapes=[pltpu.VMEM((d, width), f32)],
        ),
        out_shape=jax.ShapeDtypeStruct((d, width), bf16),
        compiler_params=pltpu.CompilerParams(dimension_semantics=("arbitrary",)),
        name="exit_grad",
    )(group, *cots, gnorm)


def run_pull_exit(group, groups, cots, weights, mixed, gate, gains):
    tokens, width = mixed.shape
    d = weights.shape[0]
    rows = tokens // groups
    nc = tokens // CHUNK

    def whole(shape, where=0):
        return pl.BlockSpec(
            shape, lambda i, g: (0,) * (len(shape) - 1) + (where,), pipeline_mode=pl.Buffered(1)
        )

    def by_row(w):
        return pl.BlockSpec((rows, w), lambda i, g: (lax.rem(g[0] + groups - i, groups), 0))

    return pl.pallas_call(
        functools.partial(pull_exit_kernel, groups),
        grid_spec=pltpu.PrefetchScalarGridSpec(
            num_scalar_prefetch=1,
            grid=(groups,),
            in_specs=[whole((rows, d))] * len(cots)
            + [
                whole((d, width), 2),
                by_row(width),
                by_row(width),
                whole(gains.shape),
            ],
            out_specs=(by_row(width), whole((nc, LANES))),
        ),
        out_shape=(
            jax.ShapeDtypeStruct((tokens, width), f32),
            jax.ShapeDtypeStruct((nc, LANES), f32),
        ),
        compiler_params=pltpu.CompilerParams(dimension_semantics=("arbitrary",)),
        name="pull_exit",
    )(group, *cots, weights, mixed, gate, gains)


def pull_gate_kernel(
    nc,
    mixed_ref,
    gate_ref,
    dgn_ref,
    sq_ref,
    dot_ref,
    gain_ref,
    cum_ref,
    rows_ref,
    act_ref,
    dmix_ref,
    dgate_ref,
    g0_ref,
    dinc_ref,
    suf_ref,
    gpart_ref,
    grad,
    total,
    gacc,
):
    i = pl.program_id(0)
    chunk = nc - 1 - i
    width = mixed_ref.shape[1]

    @pl.when(i == 0)
    def _():
        grad[...] = jnp.zeros_like(grad)
        total[...] = jnp.zeros_like(total)
        gacc[...] = jnp.zeros_like(gacc)

    scale = lax.rsqrt(column(sq_ref[pl.ds(chunk, 1), :]) / DI + norm_eps)
    inner = column(dot_ref[pl.ds(chunk, 1), :]) / DI * (scale * scale * scale)
    cum = cum_ref[...]
    last = cum[CHUNK - 1 : CHUNK]
    masks = Masks(rows_ref, nc, chunk)
    ramp = jnp.exp(cum) * masks.same(BEFORE)
    carry = jnp.exp(last) * masks.row(KEEPS)
    suf_ref[pl.ds(chunk, 1), :] = jnp.exp(total[0:1]) * masks.row(STAYS)
    total[0:1] = total[0:1] + last
    ct = lhs3(*split2(act_ref[...].T))
    for j in range(width // LANES):
        cs = slice(j * LANES, (j + 1) * LANES)
        g = gate_ref[:, cs]
        sg = sigmoid(g)
        gact = g * sg
        mixed = mixed_ref[:, cs]
        gated = mixed * gact
        dgn = dgn_ref[:, cs]
        d_gated = scale * (dgn * gain_ref[1:2, cs]) - gated * inner
        dmix = d_gated * gact
        dmix_ref[:, cs] = dmix
        dgate_ref[:, cs] = (d_gated * mixed * (sg * (1.0 + g * (1.0 - sg)))).astype(bf16)
        gacc[:, cs] = gacc[:, cs] + fold8(dgn * gated * scale)
        g0_ref[0, :, cs] = grad[:, cs]
        dw = dmix * expand(ramp, j)
        grad[:, cs] = grad[:, cs] * expand(carry, j) + dot(ct, rhs3(*split2(dw)))

    @pl.when(i == nc - 1)
    def _():
        dinc_ref[...] = grad[...]
        for j in range(width // LANES):
            cs = slice(j * LANES, (j + 1) * LANES)
            gpart_ref[j : j + 1] = jnp.sum(gacc[:, cs], axis=0, keepdims=True)
        gpart_ref[width // LANES :] = jnp.zeros((8 - width // LANES, LANES), f32)


def run_pull_gate(mixed, gate, dgn, sq, dots, gains, cum, table, act):
    tokens, width = mixed.shape
    nc = tokens // CHUNK

    def whole(shape):
        return pl.BlockSpec(shape, lambda i: (0,) * len(shape))

    def by_row(w, where=0):
        return pl.BlockSpec((CHUNK, w), lambda i: (nc - 1 - i, where))

    return pl.pallas_call(
        functools.partial(pull_gate_kernel, nc),
        grid=(nc,),
        in_specs=[
            by_row(width),
            by_row(width),
            by_row(width),
            whole(sq.shape),
            whole(dots.shape),
            whole(gains.shape),
            by_row(LANES),
            whole(table.shape),
            by_row(STATE, (width + STATE) // STATE),
        ],
        out_specs=(
            by_row(width),
            by_row(width),
            pl.BlockSpec((1, STATE, width), lambda i: (nc - 1 - i, 0, 0)),
            whole((STATE, width)),
            whole((nc, LANES)),
            whole((8, LANES)),
        ),
        out_shape=(
            jax.ShapeDtypeStruct((tokens, width), f32),
            jax.ShapeDtypeStruct((tokens, width), bf16),
            jax.ShapeDtypeStruct((nc, STATE, width), f32),
            jax.ShapeDtypeStruct((STATE, width), f32),
            jax.ShapeDtypeStruct((nc, LANES), f32),
            jax.ShapeDtypeStruct((8, LANES), f32),
        ),
        scratch_shapes=[
            pltpu.VMEM((STATE, width), f32),
            pltpu.VMEM((8, LANES), f32),
            pltpu.VMEM((8, width), f32),
        ],
        compiler_params=pltpu.CompilerParams(dimension_semantics=("arbitrary",)),
        name="pull_gate",
    )(mixed, gate, dgn, sq, dots, gains, cum, table, act)


def pull_mix_kernel(
    nc,
    per_group,
    at_ref,
    u_ref,
    act_ref,
    v_ref,
    vh_ref,
    dmix_ref,
    mixed_ref,
    del_ref,
    cum_ref,
    sig_ref,
    rows_ref,
    s0_ref,
    sin_ref,
    fin_ref,
    thr_ref,
    g0_ref,
    gin_ref,
    suf_ref,
    gain_ref,
    par_ref,
    cfa_ref,
    cfb_ref,
    dv_ref,
    ddr_ref,
    dvh_ref,
    edge_ref,
    mrow_ref,
    du,
    q1,
    q2,
    q3,
    facc,
    hacc,
    sacc,
    send,
):
    i = pl.program_id(0)
    chunk = nc - 1 - i
    width = dmix_ref.shape[1]
    cols = u_ref.shape[1]
    shifted = (q1, q2, q3)

    @pl.when(i == 0)
    def _():
        for q in shifted:
            q[...] = jnp.zeros_like(q)
        facc[...] = jnp.zeros_like(facc)
        hacc[...] = jnp.zeros_like(hacc)
        sacc[...] = jnp.zeros_like(sacc)
        send[...] = fin_ref[...]
        for j in range(width // LANES):
            cs = slice(j * LANES, (j + 1) * LANES)
            send[:, cs] = send[:, cs] + expand(thr_ref[nc : nc + 1, :], j) * sin_ref[:, cs]

    @pl.when(i > 0)
    def _():
        for q in shifted:
            q[CHUNK + 8 : CHUNK + 16] = q[8:16]

    bh, bl = split2(act_ref[:, width : width + STATE])
    ch, cl = split2(act_ref[:, width + STATE :])
    b3 = lhs3(bh, bl)
    scores_t = dot_nt(b3, rhs3_nt(ch, cl))
    cum = cum_ref[...]
    cum_t = cum.T
    r, s = ordered()
    masks = Masks(rows_ref, nc, chunk)
    allowed = (masks.seg == masks.row(SEG)) & (r <= s)
    inside, fresh = masks.same(LAST), masks.same(BACK1)
    bias = jnp.where(allowed, 0.0, NEG)
    delta = del_ref[...]
    last = cum[CHUNK - 1 : CHUNK]
    ramp = jnp.exp(cum) * masks.same(BEFORE)
    tail = jnp.exp(last - cum) * inside
    thr = thr_ref[pl.ds(chunk, 1), :]
    suf = suf_ref[pl.ds(chunk, 1), :]
    d_scores = jnp.zeros((CHUNK, CHUNK), f32)
    d_b = jnp.zeros((CHUNK, STATE), f32)
    d_c = jnp.zeros((CHUNK, STATE), f32)
    d_delta = jnp.zeros((CHUNK, LANES), f32)
    flow = jnp.zeros((CHUNK, LANES), f32)
    bound = jnp.zeros((8, LANES), f32)
    for j in range(width // LANES):
        cs = slice(j * LANES, (j + 1) * LANES)
        x = act_ref[:, cs]
        dy = dmix_ref[:, cs]
        delta_e = expand(delta, j)
        xd = x * delta_e
        dyh, dyl = split2(dy)
        zero = jnp.zeros_like(dyh)
        keep = left_half(dyh.shape)
        dyh0, dyh1 = jnp.where(keep, dyh, zero), jnp.where(keep, zero, dyh)
        dyl0, dyl1 = jnp.where(keep, dyl, zero), jnp.where(keep, zero, dyl)
        his, los, decays = [], [], []
        for h in (2 * j, 2 * j + 1):
            decay = jnp.exp(cum_t[h : h + 1, :] - cum[:, h : h + 1] + bias)
            hi, lo = split2(scores_t * decay)
            his.append(hi)
            los.append(lo)
            decays.append(decay)
        g_end = g0_ref[0, :, cs] + expand(suf, j) * gin_ref[:, cs]
        st = s0_ref[0, :, cs] + expand(thr, j) * sin_ref[:, cs]
        gh, gl = split2(g_end)
        sh, sl = split2(st)
        tail_e = expand(tail, j)
        dxd = dot(
            jnp.concatenate(his + los + his, axis=1),
            jnp.concatenate([dyh0, dyh1, dyh0, dyh1, dyl0, dyl1], axis=0),
        )
        dxd = dxd + dot(b3, rhs3(gh, gl)) * tail_e
        xdh, xdl = split2(xd)
        d_kernel = dot_nt(
            lhs3(xdh, xdl),
            jnp.concatenate(
                [rhs3_nt(dyh0, dyl0), rhs3_nt(dyh1, dyl1)],
                axis=0,
            ),
        )
        d_scores = d_scores + d_kernel[:, :CHUNK] * decays[0] + d_kernel[:, CHUNK:] * decays[1]
        d_c = d_c + dot_nt(lhs3(*split2(dy * expand(ramp, j))), rhs3_nt(sh, sl))
        d_b = d_b + dot_nt(lhs3(*split2(xd * tail_e)), rhs3_nt(gh, gl))
        skip = gain_ref[0:1, cs]
        yssm = mixed_ref[:, cs] - skip * x
        to_head = head_columns(j)
        to_head2 = jnp.concatenate([to_head, to_head], axis=0)
        d_delta = d_delta + dot(jnp.concatenate(split2(dxd * x), axis=1), to_head2)
        flow = flow + dot(jnp.concatenate(split2(dy * yssm - dxd * xd), axis=1), to_head2)
        met = fold8(g_end * send[:, cs])
        bound = bound + dot(jnp.concatenate(split2(met), axis=1), to_head2)
        send[:, cs] = st
        sacc[:, cs] = sacc[:, cs] + fold8(dy * x)
        u = u_ref[:, cs]
        sg = sigmoid(u)
        du[:, cs] = (dxd * delta_e + skip * dy) * (sg * (1.0 + u * (1.0 - sg)))
    dsh, dsl = split2(d_scores)
    d_b = d_b + dot(lhs3(dsh, dsl), rhs3(ch, cl))
    dth, dtl = split2(d_scores.T)
    d_c = d_c + dot(lhs3(dth, dtl), rhs3(bh, bl))
    for k, value in ((0, d_b), (1, d_c)):
        cs = slice(width + k * STATE, width + (k + 1) * STATE)
        u = u_ref[:, cs]
        sg = sigmoid(u)
        du[:, cs] = value * (sg * (1.0 + u * (1.0 - sg)))
    later = jnp.where(allowed, 1.0, 0.0).astype(bf16)
    later3 = jnp.concatenate([later, later, later], axis=1)
    ends = jnp.sum(bound, axis=0, keepdims=True)
    d_logdec = dot(later3, jnp.concatenate(split3(flow), axis=0)) + ends * inside
    d_logdec = d_logdec * fresh
    ddr = (d_delta + d_logdec * par_ref[1:2, :]) * sig_ref[...]
    ddr_ref[...] = pltpu.roll(ddr, at_ref[0] * per_group, 1).astype(bf16)
    hacc[0:8] = hacc[0:8] + fold8(ddr)
    hacc[8:16] = hacc[8:16] + fold8(d_logdec * par_ref[1:2, :] * delta)

    alike = [fresh, masks.same(BACK2), masks.same(BACK3)]

    def filter_of(j):
        if j < width // LANES:
            return cfa_ref[:, j * LANES : (j + 1) * LANES]
        return cfb_ref[:, j * LANES - width : (j + 1) * LANES - width]

    for j in range(cols // LANES):
        cs = slice(j * LANES, (j + 1) * LANES)
        cf = filter_of(j)
        d = du[:, cs]
        v = v_ref[:, cs].astype(f32)
        dv = cf[3:4] * d
        facc[32:40, cs] = facc[32:40, cs] + fold8(d)
        facc[24:32, cs] = facc[24:32, cs] + fold8(d * v)
        for n, q in enumerate(shifted, 1):
            q[8 : 8 + CHUNK, cs] = d * alike[n - 1]
            moved = q[8 + n : 8 + n + CHUNK, cs]
            tap = CONV - 1 - n
            dv = dv + cf[tap : tap + 1] * moved
            at = slice(8 * tap, 8 * tap + 8)
            facc[at, cs] = facc[at, cs] + fold8(moved * v)
        dv_ref[:, cs] = dv.astype(bf16)

        @pl.when(i == 0)
        def _(cs=cs, dv=dv):
            edge_ref[:, cs] = dv[CHUNK - 16 :]

    @pl.when(i == nc - 1)
    def _():
        for j in range(cols // LANES):
            cs = slice(j * LANES, (j + 1) * LANES)
            cf = filter_of(j)
            vh = vh_ref[:, cs]
            dvh = jnp.zeros((8, LANES), f32)
            for n, q in enumerate(shifted, 1):
                moved = q[n : n + 8, cs]
                tap = CONV - 1 - n
                dvh = dvh + cf[tap : tap + 1] * moved
                at = slice(8 * tap, 8 * tap + 8)
                facc[at, cs] = facc[at, cs] + moved * vh
            dvh_ref[:, cs] = dvh
        tiles = width // LANES
        mrow_ref[...] = jnp.zeros_like(mrow_ref)
        for tap in range(CONV + 1):
            for j in range(cols // LANES):
                at = tap * tiles + j if j < tiles else 5 * tiles + 8 + tap * 2 + j - tiles
                part = facc[8 * tap : 8 * tap + 8, j * LANES : (j + 1) * LANES]
                mrow_ref[at : at + 1] = jnp.sum(part, axis=0, keepdims=True)
        skips = jnp.zeros((8, LANES), f32)
        for j in range(tiles):
            part = jnp.concatenate(split3(sacc[:, j * LANES : (j + 1) * LANES]), axis=1)
            to_head = head_columns(j)
            skips = skips + dot(part, jnp.concatenate([to_head] * 3, axis=0))
        for k, part in enumerate((hacc[0:8], hacc[8:16], skips)):
            row = jnp.broadcast_to(jnp.sum(part, axis=0, keepdims=True), (8, LANES))
            at = 5 * tiles + k
            mrow_ref[at : at + 1] = pltpu.roll(row, at_ref[0] * per_group, 1)[0:1]


def run_pull_mix(
    at, per_group, u, act, v, vh, dmix, mixed, delta, cum, sig, table, s0, s_in, fin, thr, g0,
    g_in, suf, gains, par, conv_filter,
):
    tokens, cols = u.shape
    width = dmix.shape[1]
    nc = tokens // CHUNK
    taps = conv_filter.shape[0]

    def whole(shape):
        return pl.BlockSpec(
            shape, lambda i, at: (0,) * len(shape), pipeline_mode=pl.Buffered(1)
        )

    def by_row(w):
        return pl.BlockSpec((CHUNK, w), lambda i, at: (nc - 1 - i, 0))

    def states():
        return pl.BlockSpec((1, STATE, width), lambda i, at: (nc - 1 - i, 0, 0))

    def out(shape, dt=f32):
        return jax.ShapeDtypeStruct(shape, dt)

    return pl.pallas_call(
        functools.partial(pull_mix_kernel, nc, per_group),
        grid_spec=pltpu.PrefetchScalarGridSpec(
            num_scalar_prefetch=1,
            grid=(nc,),
            in_specs=[
                by_row(cols),
                by_row(cols),
                by_row(cols),
                whole(vh.shape),
                by_row(width),
                by_row(width),
                by_row(LANES),
                by_row(LANES),
                by_row(LANES),
                whole(table.shape),
                states(),
                whole(s_in.shape),
                whole(fin.shape),
                whole(thr.shape),
                states(),
                whole(g_in.shape),
                whole(suf.shape),
                whole(gains.shape),
                whole(par.shape),
                pl.BlockSpec((taps, width), lambda i, at: (0, at[0])),
                pl.BlockSpec((taps, 2 * STATE), lambda i, at: (0, DI // (2 * STATE))),
            ],
            out_specs=(
                by_row(cols),
                by_row(LANES),
                whole((8, cols)),
                whole((16, cols)),
                whole((48, LANES)),
            ),
            scratch_shapes=[
                pltpu.VMEM((CHUNK, cols), f32),
                pltpu.VMEM((CHUNK + 16, cols), f32),
                pltpu.VMEM((CHUNK + 16, cols), f32),
                pltpu.VMEM((CHUNK + 16, cols), f32),
                pltpu.VMEM((40, cols), f32),
                pltpu.VMEM((16, LANES), f32),
                pltpu.VMEM((8, width), f32),
                pltpu.VMEM((STATE, width), f32),
            ],
        ),
        out_shape=(
            out((tokens, cols), bf16),
            out((tokens, LANES), bf16),
            out((8, cols)),
            out((16, cols)),
            out((48, LANES)),
        ),
        compiler_params=pltpu.CompilerParams(dimension_semantics=("arbitrary",)),
        name="pull_mix",
    )(
        at, u, act, v, vh, dmix, mixed, delta, cum, sig, table, s0, s_in, fin, thr, g0, g_in, suf,
        gains, par, conv_filter, conv_filter,
    )


def scatter_kernel(n_dp, n_ctx, n_z, ring, widths, *refs):
    ng = len(widths)
    refs = list(refs)

    def take(n):
        return [refs.pop(0) for _ in range(n)]

    (dn_ref,), parts, (small_ref,) = take(1), take(ng), take(1)
    (dno_ref,), outs, (shared_ref, smalls_ref) = take(1), take(ng - 1), take(2)
    lands, qs, temps, opps, fins = take(ng), take(ng), take(ng), take(ng), take(ng)
    zsh, acc_sh, zland, zsum, sland, ssum, lo, far, near, comb = take(10)
    c_send, c_recv, o_send, o_recv, f_send, f_recv, g_send, g_recv, h_send, h_recv = take(10)
    s_send, s_recv, t_send, t_recv, x_send, x_recv, y_send, y_recv, n_send, n_recv = take(10)
    own = [zsh] + outs

    z, d, c = lax.axis_index("tensor"), lax.axis_index("dp"), lax.axis_index("ctx")
    pos = pick(d, [ring.index(i) for i in range(n_dp)])
    at = [pick(lax.rem(pos + r, n_dp), ring) for r in range(n_dp)]
    nxt, prv = at[1], at[n_dp - 1]
    n_plane = n_dp * n_ctx
    wr = parts[0].shape[0] // n_plane
    rows = dno_ref.shape[0]
    zc = lo.shape[1]
    zr = rows // zc
    step = 16
    mine = d * n_ctx + c

    def remote(src, dst, send, recv, **where):
        return pltpu.make_async_remote_copy(
            src, dst, send, recv, device_id=where, device_id_type=MESH
        )

    def z_at(k):
        return lax.rem(z + k, n_z)

    def c_at(k):
        return lax.rem(c + k, n_ctx)

    peers = [(at[r], c_at(s)) for r in range(n_dp) for s in range(n_ctx) if r or s]
    bar = pltpu.get_barrier_semaphore()
    for dd, cc in peers:
        pl.semaphore_signal(bar, device_id={"dp": dd, "ctx": cc}, device_id_type=MESH)
    for k in range(1, n_z):
        pl.semaphore_signal(bar, device_id={"tensor": z_at(k)}, device_id_type=MESH)
    pl.semaphore_wait(bar, len(peers) + n_z - 1)

    def ctx_copy(g, r, s):
        return remote(
            parts[g].at[pl.ds(pl.multiple_of((at[r] * n_ctx + c_at(s)) * wr, step), wr)],
            lands[g].at[s - 1, r],
            c_send.at[g, s - 1, r],
            c_recv.at[g, s - 1, r],
            ctx=c_at(s),
        )

    cut = [w // 2 // LANES * LANES for w in widths]

    def side(g, h):
        return pl.ds(0, cut[g]) if h == 0 else pl.ds(cut[g], widths[g] - cut[g])

    def opp_copy(g, h):
        return remote(
            qs[g].at[1, :, side(g, h)],
            opps[g].at[:, side(g, h)],
            o_send.at[g, h],
            o_recv.at[g, h],
            dp=nxt if h == 0 else prv,
        )

    def fin_copy(g, way, h):
        return remote(
            qs[g].at[2 * way, :, side(g, h)],
            fins[g].at[way, :, side(g, h)],
            f_send.at[g, way, h],
            f_recv.at[g, way, h],
            dp=nxt if way == 0 else prv,
        )

    def small_copy(i):
        dd, cc = peers[i]
        return remote(small_ref, sland.at[i], s_send.at[i], s_recv.at[i], dp=dd, ctx=cc)

    def small_z(k, src):
        return remote(
            ssum, smalls_ref.at[src], t_send.at[k - 1], t_recv.at[k - 1], tensor=z_at(k)
        )

    def shared_z(k):
        return remote(
            acc_sh.at[z_at(k)], zland.at[k - 1], x_send.at[k - 1], x_recv.at[k - 1], tensor=z_at(k)
        )

    def shared_back(k, src):
        return remote(
            zsum, shared_ref.at[mine, src], y_send.at[k - 1], y_recv.at[k - 1], tensor=z_at(k)
        )

    def shared_dp(r, src):
        return remote(
            shared_ref.at[mine],
            shared_ref.at[src * n_ctx + c],
            g_send.at[r - 1],
            g_recv.at[r - 1],
            dp=at[r],
        )

    def shared_ctx(r, s, src):
        return remote(
            shared_ref.at[at[r] * n_ctx + c],
            shared_ref.at[at[r] * n_ctx + src],
            h_send.at[r, s - 1],
            h_recv.at[r, s - 1],
            ctx=c_at(s),
        )

    outer = (z == 0) | (z == n_z - 1)
    inner = (z > 0) & (z < n_z - 1)
    mate = pick(z, [1, 0, 3, 2])
    far_mate, far_z = n_z - 1 - mate, n_z - 1 - z

    def dn_at(block, k):
        return pl.ds(pl.multiple_of(block * rows + k * zr, step), zr)

    def lo_copy(n, k):
        block = (far_z, far_mate, mate)[n]
        return remote(
            dn_ref.at[dn_at(block, k)], lo.at[n, k], n_send.at[n, k], n_recv.at[n, k], tensor=mate
        )

    def near_copy(k):
        return remote(
            dn_ref.at[dn_at(mate, k)], near.at[k], n_send.at[3, k], n_recv.at[3, k], tensor=mate
        )

    def comb_copy(n, k):
        return remote(
            comb.at[n, k],
            far.at[k],
            n_send.at[4 + n, k],
            n_recv.at[4, k],
            tensor=(far_mate, far_z)[n],
        )

    for g in range(ng):
        for s in range(1, n_ctx):
            for r in range(n_dp):
                ctx_copy(g, r, s).start()

    @pl.when(outer)
    def _():
        for k in range(zc):
            lo_copy(0, k).start()

    @pl.when(inner)
    def _():
        for k in range(zc):
            near_copy(k).start()

    for i in range(len(peers)):
        small_copy(i).start()

    def by_rows(fn):
        def body(i, carry):
            fn(pl.multiple_of(i * step, step))
            return carry

        lax.fori_loop(0, wr // step, body, 0)

    def first(g):
        for s in range(1, n_ctx):
            for r in range(n_dp):
                ctx_copy(g, r, s).wait_recv()

        def body(row):
            for r in range(n_dp):
                base = pl.multiple_of(mine_rows[r] + row, step)
                value = parts[g][pl.ds(base, step)].astype(f32)
                for s in range(n_ctx - 1):
                    value = value + lands[g][s, r, pl.ds(row, step)].astype(f32)
                if r == 0:
                    own[g][pl.ds(row, step)] = value
                else:
                    qs[g][r - 1, pl.ds(row, step)] = value.astype(qs[g].dtype)
                if r == 1:
                    temps[g][pl.ds(row, step), : cut[g]] = value[:, : cut[g]]
                if r == n_dp - 1:
                    temps[g][pl.ds(row, step), cut[g] :] = value[:, cut[g] :]

        by_rows(body)

    mine_rows = [(at[r] * n_ctx + c) * wr for r in range(n_dp)]

    def send_first(g):
        for h in range(2):
            opp_copy(g, h).start()
        fin_copy(g, 0, 1).start()
        fin_copy(g, 1, 0).start()

    def second(g):
        for h in range(2):
            opp_copy(g, h).wait_recv()

        def body(row):
            at_rows = pl.ds(row, step)
            value = temps[g][at_rows] + opps[g][at_rows].astype(f32)
            qs[g][0, at_rows, : cut[g]] = value[:, : cut[g]].astype(qs[g].dtype)
            qs[g][2, at_rows, cut[g] :] = value[:, cut[g] :].astype(qs[g].dtype)

        by_rows(body)

    def send_second(g):
        fin_copy(g, 0, 0).start()
        fin_copy(g, 1, 1).start()

    def third(g):
        for way in range(2):
            for h in range(2):
                fin_copy(g, way, h).wait_recv()

        def body(row):
            at_rows = pl.ds(row, step)
            own[g][at_rows] = (
                own[g][at_rows] + fins[g][0, at_rows].astype(f32) + fins[g][1, at_rows].astype(f32)
            )

        by_rows(body)

    def combine(n, k):
        @pl.when(inner)
        def _():
            lo_copy(n, k).wait_recv()
            block = (far_mate, far_z)[n]
            comb[n, k] = (dn_ref[dn_at(block, k)].astype(f32) + lo[n, k].astype(f32)).astype(bf16)

        @pl.when(outer)
        def _():
            lo_copy(n, k).wait_send()
            lo_copy(n + 1, k).start()

    def send_combined(n, k):
        @pl.when(inner)
        def _():
            comb_copy(n, k).start()

    def small_sum():
        for i in range(len(peers)):
            small_copy(i).wait_recv()
        total = small_ref[...]
        for i in range(len(peers)):
            total = total + sland[i]
        ssum[...] = total
        smalls_ref[z] = total

    def shared_split():
        for k in range(n_z):
            acc_sh[k] = zsh[k * quarter : (k + 1) * quarter]

    def shared_sum():
        for k in range(1, n_z):
            shared_z(k).wait_recv()
        total = acc_sh[z]
        for k in range(1, n_z):
            total = total + zland[k - 1]
        zsum[...] = total.astype(bf16)
        shared_ref[mine, z] = total.astype(bf16)

    quarter = wr // n_z
    first(0)
    first(1)
    send_first(0)
    first(2)
    small_sum()
    second(0)
    send_first(1)
    send_second(0)
    for k in range(1, n_z):
        small_z(k, z).start()
    first(3)
    combine(0, 0)
    third(0)
    shared_split()
    send_first(2)
    send_combined(0, 0)
    second(1)
    for k in range(1, n_z):
        shared_z(k).start()
    send_second(1)
    send_first(3)
    combine(0, 1)
    second(2)
    send_combined(0, 1)
    send_second(2)
    shared_sum()
    combine(1, 0)
    for k in range(1, n_z):
        shared_back(k, z).start()
    third(1)
    send_combined(1, 0)
    second(3)
    send_second(3)
    for k in range(1, n_z):
        shared_back(k, z_at(n_z - k)).wait_recv()
    combine(1, 1)
    for r in range(1, n_dp):
        shared_dp(r, d).start()
    for s in range(1, n_ctx):
        shared_ctx(0, s, c).start()
    third(2)
    send_combined(1, 1)
    third(3)
    for r in range(1, n_dp):
        shared_dp(r, at[n_dp - r]).wait_recv()
    for r in range(1, n_dp):
        for s in range(1, n_ctx):
            shared_ctx(r, s, c).start()
    for k in range(1, n_z):
        small_z(k, z_at(n_z - k)).wait_recv()
    for k in range(zc):
        at_rows = pl.ds(k * zr, zr)
        dno_ref[at_rows] = dn_ref[dn_at(z, k)].astype(f32)

        @pl.when(outer)
        def _(k=k, at_rows=at_rows):
            near_copy(k).wait_recv()
            dno_ref[at_rows] = dno_ref[at_rows] + near[k].astype(f32)

        @pl.when(inner)
        def _(k=k, at_rows=at_rows):
            lo_copy(2, k).wait_recv()
            dno_ref[at_rows] = dno_ref[at_rows] + lo[2, k].astype(f32)

        comb_copy(0, k).wait_recv()
        dno_ref[at_rows] = dno_ref[at_rows] + far[k].astype(f32)
    for r in range(n_dp):
        for s in range(1, n_ctx):
            shared_ctx(r, s, c_at(n_ctx - s)).wait_recv()

    for g in range(ng):
        for s in range(1, n_ctx):
            for r in range(n_dp):
                ctx_copy(g, r, s).wait_send()
        for h in range(2):
            opp_copy(g, h).wait_send()
            for way in range(2):
                fin_copy(g, way, h).wait_send()

    @pl.when(outer)
    def _():
        for k in range(zc):
            lo_copy(2, k).wait_send()

    @pl.when(inner)
    def _():
        for k in range(zc):
            near_copy(k).wait_send()
            for n in range(2):
                comb_copy(n, k).wait_send()

    for i in range(len(peers)):
        small_copy(i).wait_send()
    for k in range(1, n_z):
        small_z(k, z).wait_send()
        shared_z(k).wait_send()
        shared_back(k, z).wait_send()
    for r in range(1, n_dp):
        shared_dp(r, d).wait_send()
    for r in range(n_dp):
        for s in range(1, n_ctx):
            shared_ctx(r, s, c).wait_send()


def scatter_all(dims, d_normed, parts, small):
    n_dp, n_ctx, n_z, ring = dims
    n_plane = n_dp * n_ctx
    widths = [p.shape[1] for p in parts]
    ng = len(parts)
    wr = parts[0].shape[0] // n_plane
    rows, d = d_normed.shape[0] // n_z, d_normed.shape[1]
    zc = 2
    dma = pltpu.SemaphoreType.DMA
    vmem = pltpu.VMEM
    quarter = wr // n_z

    def out(*shape):
        return jax.ShapeDtypeStruct(shape, f32)

    outs = (
        [out(rows, d)]
        + [out(wr, w) for w in widths[1:]]
        + [
            jax.ShapeDtypeStruct((n_plane, n_z, quarter, widths[0]), bf16),
            out(n_z, *small.shape),
        ]
    )
    scratch = (
        [vmem((n_ctx - 1, n_dp, wr, p.shape[1]), p.dtype) for p in parts]
        + [vmem((3, wr, p.shape[1]), p.dtype) for p in parts]
        + [vmem((wr, w), f32) for w in widths]
        + [vmem((wr, p.shape[1]), p.dtype) for p in parts]
        + [vmem((2, wr, p.shape[1]), p.dtype) for p in parts]
        + [
            vmem((wr, widths[0]), f32),
            vmem((n_z, quarter, widths[0]), f32),
            vmem((n_z - 1, quarter, widths[0]), f32),
            vmem((quarter, widths[0]), bf16),
            vmem((n_plane - 1,) + small.shape, f32),
            vmem(small.shape, f32),
            vmem((3, zc, rows // zc, d), bf16),
            vmem((zc, rows // zc, d), bf16),
            vmem((zc, rows // zc, d), bf16),
            vmem((2, zc, rows // zc, d), bf16),
        ]
        + [dma((ng, n_ctx - 1, n_dp))] * 2
        + [dma((ng, 2))] * 2
        + [dma((ng, 2, 2))] * 2
        + [dma((n_dp - 1,))] * 2
        + [dma((n_dp, n_ctx - 1))] * 2
        + [dma((n_plane - 1,))] * 2
        + [dma((n_z - 1,))] * 6
        + [dma((6, zc)), dma((5, zc))]
    )
    return pl.pallas_call(
        functools.partial(scatter_kernel, n_dp, n_ctx, n_z, ring, widths),
        out_shape=tuple(outs),
        in_specs=[pl.BlockSpec(memory_space=pltpu.VMEM)] * (ng + 2),
        out_specs=tuple([pl.BlockSpec(memory_space=pltpu.VMEM)] * len(outs)),
        scratch_shapes=scratch,
        compiler_params=pltpu.CompilerParams(collective_id=3, has_side_effects=True),
        name="scatter_all",
    )(d_normed, *parts, small)


def update_kernel(
    tiles, dn_ref, x_ref, cot_ref, ng_ref, *refs
):
    refs = list(refs)

    def take(n):
        return [refs.pop(0) for _ in range(n)]

    parts = take(4)
    gate_g, inner_g, exit_g, shared_g, smalls = take(5)
    entry, leave, shared, norm, conv, head, gated = (take(3) for _ in range(7))
    y_out, ig_out = take(2)
    n_out, e_out, s_out, c_out, h_out, g_out, l_out = (take(4) for _ in range(7))
    e_buf, e_new, e_in, e_back = take(4)
    i = pl.program_id(0)

    def fetch(n, which):
        return pltpu.make_async_copy(
            entry[n].at[:, which, :], e_buf.at[n, which], e_in.at[n, which]
        )

    def store(n, which):
        return pltpu.make_async_copy(
            e_new.at[n, which], e_out[n].at[:, which, :], e_back.at[n, which]
        )

    @pl.when(i == 0)
    def _():
        for which in range(2):
            for n in range(3):
                fetch(n, which).start()

    for which, grad in ((0, gate_g), (1, inner_g)):

        @pl.when(i == which + 1)
        def _(which=which, grad=grad):
            for n in range(3):
                fetch(n, which).wait()
            own = [e_buf[n, which] for n in range(3)]
            new = adamw(own[0], grad[...], own[1], own[2], rate_matrix, decay_matrix)
            for n in range(4):
                e_new[n, which] = new[n]

        @pl.when(i == which + 2)
        def _(which=which):
            for n in range(4):
                store(n, which).start()

    @pl.when(i == pl.num_programs(0) - 1)
    def _():
        for which in range(2):
            for n in range(4):
                store(n, which).wait()


    def put(outs, values, at):
        for ref, value in zip(outs, values, strict=True):
            ref[at] = value

    at = (slice(None), slice(None))
    own = [ref[at] for ref in leave]
    put(l_out, adamw(own[0], exit_g[...], own[1], own[2], rate_matrix, decay_matrix), at)
    n = shared[0].shape[0]
    g = shared_g[...].astype(f32).T[:n]
    own = [ref[at] for ref in shared]
    put(s_out, adamw(own[0], g, own[1], own[2], rate_matrix, decay_matrix), at)

    @pl.when(i < 4)
    def _():
        x = x_ref[...].astype(f32)
        y = x
        for part in parts:
            y = y + part[...].astype(f32)
        y_out[...] = y.astype(bf16)
        scale = lax.rsqrt(jnp.mean(x * x, axis=-1, keepdims=True) + norm_eps)
        d_scaled = dn_ref[...] * ng_ref[...]
        inner = jnp.mean(d_scaled * x, axis=-1, keepdims=True) * (scale * scale * scale)
        value = cot_ref[...].astype(f32) + scale * d_scaled - x * inner
        across = value.shape[1] // LANES
        for k in range(across):
            at = (pl.ds(k, value.shape[0], stride=across), slice(None))
            ig_out[at] = value[:, k * LANES : (k + 1) * LANES]

    @pl.when(i == 0)
    def _():
        n_z = smalls.shape[0]

        def summed(lo, hi):
            out = smalls[0, lo:hi]
            for z in range(1, n_z):
                out = out + smalls[z, lo:hi]
            return out

        for z in range(n_z):
            g_out[0][z * tiles : (z + 1) * tiles] = smalls[z, :tiles]
            for tap in range(CONV + 1):
                for k in range(tiles):
                    at = 8 + tap * tiles + k
                    to = (z * tiles + k) * LANES
                    c_out[0][tap : tap + 1, to : to + LANES] = smalls[z, at : at + 1]
        bc = summed(16 + 5 * tiles, 26 + 5 * tiles)
        for tap in range(CONV + 1):
            for k in range(2):
                to = (n_z * tiles + k) * LANES
                c_out[0][tap : tap + 1, to : to + LANES] = bc[2 * tap + k : 2 * tap + k + 1]
        heads = summed(8 + 5 * tiles, 11 + 5 * tiles)
        h_out[0][...] = heads[:, : head[0].shape[1]]
        n_out[0][...] = summed(56, 56 + norm[0].shape[0])
        for outs, old in ((n_out, norm), (c_out, conv), (h_out, head), (g_out, gated)):
            g = outs[0][...]
            new = adamw(old[0][...], g, old[1][...], old[2][...], rate_vector, 0.0)
            put(outs, new, at_all)


at_all = (slice(None), slice(None))


def run_update(dn, x, cot, ng, parts, grads, smalls, entry, leave, shared, norm, conv, head, gated):
    steps = 6
    tiles = leave[0].shape[1] // LANES
    rows = leave[0].shape[0] // steps
    d = dn.shape[1]
    quarter = dn.shape[0] // 4
    across = d // LANES

    def clip(i):
        return jnp.minimum(i, 3)

    def whole(a):
        return pl.BlockSpec(a.shape, lambda i: (0,) * a.ndim)

    def by_row(a, n):
        return pl.BlockSpec((n, a.shape[1]), lambda i: (i, 0))

    token = pl.BlockSpec((quarter, d), lambda i: (clip(i), 0))
    columns = pl.BlockSpec((shared[0].shape[0], d // steps), lambda i: (0, i))
    e_spec = pl.BlockSpec(memory_space=pl.ANY)
    l_spec = by_row(leave[0], rows)
    groups = (
        (norm, whole(norm[0])),
        (entry, e_spec),
        (shared, columns),
        (conv, whole(conv[0])),
        (head, whole(head[0])),
        (gated, whole(gated[0])),
        (leave, l_spec),
    )
    return pl.pallas_call(
        functools.partial(update_kernel, tiles),
        grid=(steps,),
        in_specs=[token, token, token, whole(ng)]
        + [token] * 4
        + [whole(grads[0])] * 2
        + [l_spec, pl.BlockSpec((d // steps, grads[3].shape[1]), lambda i: (i, 0)), whole(smalls)]
        + [e_spec] * 3
        + [l_spec] * 3
        + [columns] * 3
        + [whole(norm[0])] * 3
        + [whole(conv[0])] * 3
        + [whole(head[0])] * 3
        + [whole(gated[0])] * 3,
        out_specs=(token, pl.BlockSpec((quarter * across, LANES), lambda i: (clip(i), 0)))
        + tuple(spec for _, spec in groups for _ in range(4)),
        out_shape=(
            jax.ShapeDtypeStruct(x.shape, bf16),
            jax.ShapeDtypeStruct((x.shape[0] * across, LANES), f32),
        )
        + tuple(jax.ShapeDtypeStruct(a[0].shape, f32) for a, _ in groups for _ in range(4)),
        scratch_shapes=[
            pltpu.VMEM((3, 2) + leave[0].shape, f32),
            pltpu.VMEM((4, 2) + leave[0].shape, f32),
            pltpu.SemaphoreType.DMA((3, 2)),
            pltpu.SemaphoreType.DMA((4, 2)),
        ],
        compiler_params=pltpu.CompilerParams(dimension_semantics=("arbitrary",)),
        name="update",
    )(dn, x, cot, ng, *parts, *grads, smalls, *entry, *leave, *shared, *norm, *conv, *head, *gated)


def shift(block, axis, by):
    n = lax.axis_size(axis)
    return lax.ppermute(block, axis, [(i, i + by) for i in range(n) if 0 <= i + by < n])


def turn(block, axis, by):
    n = lax.axis_size(axis)
    return lax.ppermute(block, axis, [(i, (i + by) % n) for i in range(n)])


def adamw(weight, grad, first, second, rate, decay):
    first_new = beta_first * first + (1.0 - beta_first) * grad
    second_new = beta_second * second + (1.0 - beta_second) * grad * grad
    first_hat = first_new / (1.0 - beta_first**STEP)
    second_hat = second_new / (1.0 - beta_second**STEP)
    weight_new = weight - rate * (first_hat / (jnp.sqrt(second_hat) + adam_eps) + decay * weight)
    return (grad, weight_new, first_new, second_new)


def per_lane(row):
    return jnp.repeat(row, HEAD_DIM, axis=-1)


def state_scan(through, final, axis, reverse):
    n, mine = lax.axis_size(axis), lax.axis_index(axis)
    if n == 2:
        moved = shift(final, axis, -1 if reverse else 1)
        return moved
    finals = lax.all_gather(final, axis)
    rates = lax.all_gather(through, axis)
    acc = jnp.zeros_like(final)
    for k in range(n - 1):
        at = n - 1 - k if reverse else k
        nxt = rates[at] * acc + finals[at]
        acc = jnp.where(at > mine if reverse else at < mine, nxt, acc)
    return acc


def local(
    dims,
    block_in,
    cotangent,
    segments,
    norm_gain,
    inward_weight,
    shared_weight,
    conv_filter,
    head_params,
    gated_gain,
    exit_weight,
    norm_first,
    norm_second,
    entry_first,
    entry_second,
    shared_first,
    shared_second,
    filter_first,
    filter_second,
    head_first,
    head_second,
    gated_first,
    gated_second,
    exit_first,
    exit_second,
):
    group = lax.axis_index("tensor")
    groups = lax.axis_size("tensor")
    per_group = HEADS // groups
    width = DI // groups
    rows, _, d = block_in.shape
    tokens = rows * groups
    nc = tokens // CHUNK
    x, cot = block_in[:, 0], cotangent[:, 0]
    at = jnp.stack([group, (lax.axis_index("ctx") > 0).astype(jnp.int32)]).astype(jnp.int32)

    seg = segments.reshape(nc, CHUNK)
    hp = jnp.pad(head_params, ((0, 5), (0, LANES - HEADS)))
    gg = gated_gain.reshape(-1, LANES)
    normed_own, w_own, ws = run_prep(
        x, norm_gain[None], inward_weight, exit_weight, shared_weight.T
    )
    normed, weights, halo, pseg = gather_all(dims, normed_own, w_own, seg)

    first = lax.optimization_barrier((cot, halo))[0]
    lower, upper = [first], [first]
    for _ in range(1, groups):
        lower.append(shift(lower[-1], "tensor", 1))
        upper.append(shift(upper[-1], "tensor", -1))
    cots = [cot] + lower[1:] + upper[1:]

    gate, v, u, act, delta, cum, sig, s0, fin, thr, vh, table, par, gains = run_entry(
        at, per_group, normed, weights, ws, halo, seg, pseg, hp, gg, conv_filter
    )
    through = per_lane(thr[nc : nc + 1, :per_group])
    s_in = state_scan(through, fin, "ctx", False)
    mixed, sq = run_mix(act, delta, cum, table, s0, s_in, thr, gate, gains)
    group_at = at[:1]
    dgn, dots = run_pull_exit(group_at, groups, cots, weights, mixed, gate, gains)
    sq, dots = all_sum(groups, 1, sq, dots)
    gnorm, *out_parts = run_exit(group_at, groups, mixed, gate, sq, gains, weights)
    out_parts = [out_parts[0]] + [turn(out_parts[k], "tensor", k) for k in range(1, groups)]
    exit_part = run_exit_grad(group_at, groups, cots, gnorm)
    dmix, d_gate, g0, d_inc, suf, gpart = run_pull_gate(
        mixed, gate, dgn, sq, dots, gains, cum, table, act
    )
    g_in = state_scan(through, d_inc, "ctx", True)
    d_v, d_raw, d_vh, edge, mrows = run_pull_mix(
        at, per_group, u, act, v, vh, dmix, mixed, delta, cum, sig, table, s0, s_in, fin, thr, g0,
        g_in, suf, gains, par, conv_filter,
    )
    from_next = shift(d_vh, "ctx", -1)
    edge = edge.at[8:].add(from_next).astype(bf16)
    d_v = lax.dynamic_update_slice_in_dim(d_v, edge, tokens - 16, 0)

    d_all = jnp.concatenate([d_gate, d_v, d_raw], axis=1)
    back = (
        lax.dot_general(d_all[:, : 2 * width], weights[:, : 2 * width], NT, preferred_element_type=f32)
        + jnp.dot(d_all[:, 2 * width :], ws, preferred_element_type=f32)
    ).astype(bf16)
    w_part = lax.dot_general(
        normed, d_all, (((0,), (0,)), ((), ())), preferred_element_type=f32
    )
    w_all = jnp.concatenate([weights[:, : 2 * width], ws.T], axis=1)
    norm_part = jnp.sum(w_part * w_all.astype(f32), axis=1) / norm_gain
    shared_part = w_part[:, 2 * width :]
    w_part = w_part.astype(bf16)
    small = jnp.concatenate(
        [gpart, mrows, jnp.pad(norm_part, (0, 16 * LANES - d)).reshape(16, LANES)]
    )
    d_normed, exit_grad, grad_gate, grad_inner, shared_sum, smalls = scatter_all(
        dims,
        back,
        [shared_part, exit_part, w_part[:, :width], w_part[:, width : 2 * width]],
        small,
    )

    def rows_of(a):
        return a.reshape(-1, LANES)

    out, d_in, *sets = run_update(
        d_normed,
        x,
        cot,
        norm_gain[None],
        out_parts,
        [grad_gate, grad_inner, exit_grad, shared_sum.reshape(d, -1)],
        smalls,
        [inward_weight, entry_first, entry_second],
        [exit_weight, exit_first, exit_second],
        [a.T for a in (shared_weight, shared_first, shared_second)],
        [rows_of(a) for a in (norm_gain, norm_first, norm_second)],
        [conv_filter, filter_first, filter_second],
        [head_params, head_first, head_second],
        [rows_of(a) for a in (gated_gain, gated_first, gated_second)],
    )
    n_set, e_set, s_set, c_set, h_set, g_set, l_set = (sets[4 * k : 4 * k + 4] for k in range(7))
    return (
        out[:, None],
        d_in.reshape(rows, 1, d),
        *(a.reshape(-1) for a in n_set),
        *e_set,
        *(a.T for a in s_set),
        *c_set,
        *h_set,
        *(a.reshape(-1) for a in g_set),
        *l_set,
    )


def solution(mesh):
    n_dp, n_ctx, n_z = (mesh.shape[a] for a in ("dp", "ctx", "tensor"))
    ring = [0, 1, 3, 2] if n_ctx == 2 and n_dp == 4 else list(range(n_dp))
    dims = (n_dp, n_ctx, n_z, ring)
    token = P(("ctx", "tensor"), "dp", None)
    entry = P(("dp", "ctx"), None, "tensor")
    leave = P(("dp", "ctx"), "tensor")
    rep = P()
    return jax.shard_map(
        functools.partial(local, dims),
        mesh=mesh,
        in_specs=(
            token, token, P("dp", "ctx"), rep, entry, rep, rep, rep, rep, leave,
            rep, rep, entry, entry, rep, rep, rep, rep, rep, rep, rep, rep, leave, leave,
        ),
        out_specs=(token, token)
        + (rep,) * 4 + (entry,) * 4 + (rep,) * 16 + (leave,) * 4,
        check_vma=False,
    )
```
